256 devices in a mesh: dp: 8 (over x, core), expert: 32 (over y, z).
Axes of the slice: x: 4, y: 4, z: 8, core: 2. Of those that a mesh axis runs over, the one named last changes fastest.
Arguments:
- queries: bfloat16 [2048, 16, 3072], P('expert', 'dp'), may hold values from -256 to 256
- key_nope: bfloat16 [2048, 16, 2048], P('expert', 'dp'), may hold values from -4 to 4
- key_rope: bfloat16 [2048, 16, 64], P('expert', 'dp'), may hold values from -4 to 4
- values: bfloat16 [2048, 16, 2048], P('expert', 'dp'), may hold values from -6 to 6
- residual: bfloat16 [2048, 16, 2048], P('expert', 'dp'), may hold values from -6 to 6
- segments: int32 [16, 2048], P('dp'), may hold values from 0 to 1, never falling along the last dimension, each value on 1 to 1536 neighbouring positions
- out_proj: bfloat16 [2048, 2048], P(('dp', 'expert')), may hold values from -0.125 to 0.125
- norm_gain: bfloat16 [2048], replicated, may hold values from 0.5 to 1.5
- expert_gate: bfloat16 [32, 2048, 704], P('expert'), may hold values from -0.125 to 0.125
- expert_up: bfloat16 [32, 2048, 704], P('expert'), may hold values from -0.125 to 0.125
- expert_down: bfloat16 [32, 704, 2048], P('expert'), may hold values from -0.21875 to 0.21875
- routes: int32 [8, 32, 128, 6], P('dp', 'expert'), may hold values from 0 to 31, all different within a row; in each aligned block of 128 rows (0 to 127, 128 to 255, ..., all dimensions but the last counted through in order) at most 36 rows name the same one
- route_weights: float32 [8, 32, 128, 6], P('dp', 'expert'), may hold values from 0.1 to 0.6
Outputs:
- layer_out: bfloat16 [2048, 16, 2048], P('expert', 'dp')
The draws below stay inside these ranges and needn't reach their ends.
Inputs may be any that keep to these rules, and one draw needn't show every extreme that they name: `routes`: each row names 6 different experts; within the rows of one device no expert is named more than 36 times.
All inputs are finite; a program needn't handle non-finite values.
Results may differ from the reference program's by a relative error of at most 0.0049.
Values may be sent and summed in bfloat16 or wider, within the bound.
A program may use at most 128 MiB of HBM per device.

```python
import math
import jax
import jax.numpy as jnp
import numpy as np
from jax import lax

D = 2048
HEADS = 16
NOPE = 128
ROPE = 64
V_DIM = 128
FF_E = 704
TOP = 6
STREAMS = 2
DOCS = 2
TOK_HALF = 64
QK_DIM = 192
EXPERTS = 32
LENGTH = 2048
S_ALL = 16
TOK_DEV = 128
MOST = 36
DOC_MOST = 1536
N_DP = 8
N_EXPERT = 32


def key_parts(key):
    nope_part = jnp.clip(jax.random.normal(jax.random.fold_in(key, 11), (LENGTH, S_ALL, HEADS * NOPE), jnp.float32), -4.0, 4.0)
    rope_part = jnp.clip(jax.random.normal(jax.random.fold_in(key, 12), (LENGTH, S_ALL, ROPE), jnp.float32), -4.0, 4.0)
    return (nope_part, rope_part)


def draw_key_nope(key, part):
    return key_parts(key)[0].astype(jnp.bfloat16)


def draw_key_rope(key, part):
    return key_parts(key)[1].astype(jnp.bfloat16)


def draw_queries(key, part):
    drawn = jnp.clip(jax.random.normal(jax.random.fold_in(key, 15), (LENGTH, S_ALL, HEADS * QK_DIM), jnp.float32), -6.0, 6.0)
    return drawn.astype(jnp.bfloat16)


def steps_of(key, dims, shards, smallest, largest):
    def one(axis_at, shards_of):
        heights = jax.random.uniform(jax.random.fold_in(jax.random.fold_in(key, 6), axis_at), (shards_of,), jnp.float32, smallest / len(shards), largest / len(shards))
        return jnp.repeat(jnp.exp(heights), dims[axis_at] // shards_of).reshape((-1,) + (1,) * (len(dims) - axis_at - 1))

    loudness = one(*shards[0])
    for cut in shards[1:]:
        loudness = loudness * one(*cut)
    return loudness


def profile(amount, total, bound, skew):
    portions = [(1 << 20) // math.isqrt(rank ** skew) + 1 for rank in range(2, amount + 1)]
    surplus, given = total - bound - (amount - 1), [1] * (amount - 1)
    while surplus > 0:
        movable = [i for i in range(amount - 1) if given[i] < bound]
        mass, budget = sum([portions[i] for i in movable]), surplus
        for i in movable:
            more = min(bound - given[i], max(1, budget * portions[i] // mass), surplus)
            given[i] = given[i] + more
            surplus = surplus - more
    return np.array([bound] + given)


def uneven(own_key, count, total, most, lean):
    if count == 2:
        one = jax.random.randint(own_key, (), max(1, total - most), min(most, total - 1) + 1)
        return jnp.stack([one, total - one])
    sizes = jnp.asarray(profile(count, total, most, lean), jnp.int32)
    twos = (count - 1) // 2
    giver, receiver = sizes[1:1 + 2 * twos:2], sizes[2:2 + 2 * twos:2]
    slack = jnp.minimum(giver - 1, most - receiver)
    passed = jax.random.randint(jax.random.fold_in(own_key, 1), (twos,), 0, 1 << 20) % (slack + 1)
    sizes = sizes.at[1:1 + 2 * twos:2].set(giver - passed).at[2:2 + 2 * twos:2].set(receiver + passed)
    return sizes[jax.random.permutation(jax.random.fold_in(own_key, 2), count)]


def routed_block(key, own, number, rows, count, top, most, slope):
    ranking = jax.random.permutation(key, count)
    heavy_load, usual = portions_of(count, rows * top, most, slope, True), portions_of(count, rows * top, most, slope, False)
    places = jnp.arange(count)

    def named(lengths, rotation):
        used = int((lengths > 0).sum())
        fixed = max(1, used // 4)
        passed = fixed + (places - fixed + rotation * (used - fixed)) % max(1, count - fixed)
        return jnp.zeros((count,), jnp.int32).at[ranking[jnp.where(places < fixed, places, passed)]].set(jnp.asarray(lengths, jnp.int32))

    lengths = jnp.where(number % 4 == 0, named(heavy_load, number // 4), named(usual, number - number // 4 - 1))
    mixed = jax.random.permutation(jax.random.fold_in(own, 3), count)
    source_of, receiver = mixed[0:count // 2 * 2:2], mixed[1:count // 2 * 2:2]
    margin = jnp.minimum(lengths[source_of] - 1, most - lengths[receiver]) // 2
    margin = jnp.where((source_of == ranking[0]) | (receiver == ranking[0]) | (lengths[receiver] == 0), 0, jnp.maximum(margin, 0))
    passed = jax.random.randint(jax.random.fold_in(own, 4), (count // 2,), 0, 1 << 20) % (margin + 1)
    lengths = lengths.at[source_of].add(-passed).at[receiver].add(passed)
    labels = jnp.searchsorted(jnp.cumsum(lengths), jnp.arange(rows * top), side="right").astype(jnp.int32)
    grid = labels.reshape(top, rows).T
    grid = grid[jax.random.permutation(jax.random.fold_in(own, 1), rows)]
    rotation = jax.random.randint(jax.random.fold_in(own, 2), (rows, 1), 0, top)
    return jnp.take_along_axis(grid, (jnp.arange(top)[None, :] + rotation) % top, axis=1)


def portions_of(number_of, total, most, lean, full):
    loads = [(1 << 20) // math.isqrt(standing ** lean) + 1 for standing in range(1, number_of + 1)]
    largest = most if full else min(most, max(-(-total // number_of), total * loads[0] // sum(loads)))
    least = 1 if total - largest >= number_of - 1 else 0
    counts, surplus = [largest] + [least] * (number_of - 1), total - largest - least * (number_of - 1)
    while surplus > 0:
        free = [i for i in range(1, number_of) if counts[i] < largest] or [i for i in range(1, number_of) if counts[i] < most]
        pool, left = sum([loads[i] for i in free]), surplus
        for i in free:
            extra = min(most - counts[i], max(1, left * loads[i] // pool), surplus)
            counts[i] = counts[i] + extra
            surplus = surplus - extra
    return np.array(counts)


def normal_values(own_key, extent, scale, most, shards=(), held_as=jnp.bfloat16):
    values = scale * jax.random.normal(own_key, extent, jnp.float32)
    if shards:
        values = values * steps_of(own_key, extent, shards, -0.22, 0.18)
    return jnp.clip(values, -most, most).astype(held_as)


def setup_inputs(seed: int = 0) -> dict:
    streams_of = jax.random.split(jax.random.key(seed), 14)
    queries = draw_queries(jax.random.fold_in(streams_of[13], 71), 0)
    key_nope = draw_key_nope(jax.random.fold_in(streams_of[13], 71), 0)
    key_rope = draw_key_rope(jax.random.fold_in(streams_of[13], 71), 0)
    values = normal_values(streams_of[3], (LENGTH, S_ALL, HEADS * V_DIM), 1.0, 6.0, ((0, 32), (1, 8)))
    residual = normal_values(streams_of[4], (LENGTH, S_ALL, D), 1.0, 6.0, ((0, 32), (1, 8)))
    segments = jax.vmap(lambda own: jnp.searchsorted(jnp.cumsum(uneven(own, DOCS, LENGTH, DOC_MOST, 1)), jnp.arange(LENGTH), side="right"))(jax.random.split(streams_of[5], S_ALL)).reshape((S_ALL, LENGTH)).astype(jnp.int32)
    out_proj = normal_values(streams_of[6], (HEADS * V_DIM, D), (HEADS * V_DIM) ** -0.5, 0.125, ((0, 256),))
    norm_gain = jnp.clip(1.0 + 0.1 * jax.random.normal(streams_of[7], (D,), jnp.float32), 0.5, 1.5).astype(jnp.bfloat16)
    expert_gate = normal_values(streams_of[8], (EXPERTS, D, FF_E), D ** -0.5, 0.125, ((0, 32),))
    expert_up = normal_values(streams_of[9], (EXPERTS, D, FF_E), D ** -0.5, 0.125, ((0, 32),))
    expert_down = normal_values(streams_of[10], (EXPERTS, FF_E, D), FF_E ** -0.5, 0.21875, ((0, 32),))
    routes_keys = jax.random.split(jax.random.fold_in(streams_of[11], 1), N_DP * N_EXPERT * TOK_DEV // TOK_DEV)
    routes_turns = jax.random.permutation(jax.random.fold_in(streams_of[11], 3), N_DP * N_EXPERT * TOK_DEV // TOK_DEV)
    routes = jax.vmap(lambda own, number: routed_block(jax.random.fold_in(streams_of[11], 2), own, number, TOK_DEV, EXPERTS, TOP, MOST, 1))(routes_keys, routes_turns).reshape((N_DP, N_EXPERT, TOK_DEV, TOP))
    route_weights = jnp.clip(0.1 + 0.5 * jax.random.uniform(streams_of[12], (N_DP, N_EXPERT, TOK_DEV, TOP), jnp.float32) ** steps_of(streams_of[12], (N_DP, N_EXPERT, TOK_DEV, TOP), ((0, 8), (1, 32)), -0.2, 0.2), 0.1, 0.6)
    return dict(queries=queries, key_nope=key_nope, key_rope=key_rope, values=values, residual=residual, segments=segments, out_proj=out_proj, norm_gain=norm_gain, expert_gate=expert_gate, expert_up=expert_up, expert_down=expert_down, routes=routes, route_weights=route_weights)


EPSILON = 1e-06

def to_streams(block_array):
    width = block_array.shape[-1]
    shaped = block_array.reshape(N_DP, N_EXPERT, TOK_HALF, STREAMS, width)
    shaped = jnp.transpose(shaped, (1, 2, 0, 3, 4))
    return shaped.reshape(LENGTH, S_ALL, width)

def feed_forward(rows, gate_matrix, up_matrix, down_matrix):
    gate_part = jnp.dot(rows, gate_matrix, preferred_element_type=jnp.float32)
    up_part = jnp.dot(rows, up_matrix, preferred_element_type=jnp.float32)
    activated = (jax.nn.silu(gate_part) * up_part).astype(jnp.bfloat16)
    return jnp.dot(activated, down_matrix, preferred_element_type=jnp.float32).astype(jnp.bfloat16)

def attend_stream(inputs):
    query_rows, nope_rows, rope_rows, value_rows, segment_row = inputs
    query_heads = query_rows.reshape(LENGTH, HEADS, QK_DIM).astype(jnp.float32)
    key_heads = jnp.concatenate([nope_rows.reshape(LENGTH, HEADS, NOPE), jnp.broadcast_to(rope_rows[:, None, :], (LENGTH, HEADS, ROPE))], axis=2).astype(jnp.float32)
    value_heads = value_rows.reshape(LENGTH, HEADS, V_DIM).astype(jnp.float32)
    scores = jnp.einsum('qhd,khd->hqk', query_heads, key_heads) * QK_DIM ** (-0.5)
    positions = jnp.arange(LENGTH, dtype=jnp.int32)
    allowed = (positions[:, None] >= positions[None, :]) & (segment_row[:, None] == segment_row[None, :])
    scores = jnp.where(allowed[None], scores, -jnp.inf)
    row_peak = lax.optimization_barrier(jnp.max(scores, axis=2, keepdims=True))
    raised = jnp.exp(scores - row_peak)
    probs = (raised / lax.optimization_barrier(jnp.sum(raised, axis=2, keepdims=True))).astype(jnp.bfloat16)
    mixed = jnp.einsum('hqk,khd->qhd', probs.astype(jnp.float32), value_heads)
    return mixed.reshape(LENGTH, HEADS * V_DIM).astype(jnp.bfloat16)

def reference(queries, key_nope, key_rope, values, residual, segments, out_proj, norm_gain, expert_gate, expert_up, expert_down, routes, route_weights):
    inputs = (jnp.swapaxes(queries, 0, 1), jnp.swapaxes(key_nope, 0, 1), jnp.swapaxes(key_rope, 0, 1), jnp.swapaxes(values, 0, 1), segments)
    attended = lax.map(attend_stream, inputs)
    token_count = LENGTH * S_ALL
    attn_rows = jnp.swapaxes(attended, 0, 1).reshape(token_count, HEADS * V_DIM)
    projected = jnp.dot(attn_rows, out_proj, preferred_element_type=jnp.float32)
    hidden = residual.reshape(token_count, D).astype(jnp.float32) + projected
    mean_square = lax.optimization_barrier(jnp.mean(hidden * hidden, axis=1, keepdims=True))
    normed = (hidden * lax.rsqrt(mean_square + EPSILON) * norm_gain.astype(jnp.float32)).astype(jnp.bfloat16)
    chosen = to_streams(routes).reshape(token_count, TOP)
    scales = to_streams(route_weights).reshape(token_count, TOP)
    capacity = min(N_DP * N_EXPERT * MOST, token_count)
    row_ids = jnp.arange(token_count, dtype=jnp.int32)

    def one_expert(routed_total, expert_inputs):
        gate_matrix, up_matrix, down_matrix, expert_id = expert_inputs
        matches = chosen == expert_id
        picked = jnp.any(matches, axis=1)
        weight_row = lax.optimization_barrier(jnp.sum(jnp.where(matches, scales, jnp.zeros_like(scales)), axis=1))
        live_order = (jnp.cumsum(picked.astype(jnp.int32)) - 1).astype(jnp.int32)
        live_place = jnp.where(picked, live_order, capacity).astype(jnp.int32)
        source_rows = jnp.zeros((capacity,), jnp.int32).at[live_place].set(row_ids, mode='drop')
        filled = jnp.zeros((capacity,), jnp.int32).at[live_place].set(1, mode='drop')
        outputs = feed_forward(normed[source_rows], gate_matrix, up_matrix, down_matrix)
        contribution = (filled > 0)[:, None] * weight_row[source_rows][:, None] * outputs.astype(jnp.float32)
        return (routed_total.at[source_rows].add(contribution), expert_id)
    expert_ids = jnp.arange(EXPERTS, dtype=jnp.int32)
    routed_total = lax.scan(one_expert, jnp.zeros((token_count, D), jnp.float32), (expert_gate, expert_up, expert_down, expert_ids))[0]
    layer_out = (hidden + routed_total).astype(jnp.bfloat16)
    return layer_out.reshape(LENGTH, S_ALL, D)
```

```python
import functools

import jax
import jax.numpy as jnp
from jax import lax
from jax.experimental import pallas as pl
from jax.experimental.pallas import tpu as pltpu
from jax.sharding import Mesh, PartitionSpec as P

MESH = pl.DeviceIdType.MESH
DP = ("x", "core")
EXPERT = ("y", "z")

HEADS = 16
NOPE = 128
ROPE = 64
V_DIM = 128
TOP = 6


EPSILON = 1e-06
QUERY_BLOCK = 512


def side_by_side(arrays, axis, split_dim, concat_dim, along):
    widths = [a.shape[along] for a in arrays]
    both = jnp.concatenate(arrays, axis=along)
    result = lax.all_to_all(both, axis, split_axis=split_dim, concat_axis=concat_dim, tiled=True)
    return tuple(jnp.split(result, [sum(widths[:k]) for k in range(1, len(widths))], axis=along))


def moe_kernel(axis_size, x_ref, hid_ref, wt_ref, wi_hbm, wd_hbm, out_ref,
               xbuf, acc, act, wi, wd, rbuf, lbuf, start_sem, send_sem, recv_sem, wsem):
    n = axis_size
    half_n = n // 2
    z = lax.axis_index("z")
    right = {"z": lax.rem(z + 1, n)}
    left = {"z": lax.rem(z + n - 1, n)}
    rows = x_ref.shape[0]
    half = rows // 2
    pieces, count, depth, ff = wi_hbm.shape[:3] + (wi_hbm.shape[3] // 2,)
    sent = 2 * half_n - 1

    def slot(d):
        return lax.rem(z + 2 * n - d, n)

    def part(c):
        return pl.ds(pl.multiple_of(c * half, half), half)

    def fetch(k, carry):
        for i in range(pieces):
            span = pl.ds(i * depth, depth)
            pltpu.make_async_copy(wi_hbm.at[i, k], wi.at[k, span], wsem.at[k, 0]).start()
            pltpu.make_async_copy(wd_hbm.at[i, k], wd.at[k, :, span], wsem.at[k, 1]).start()
        return carry

    lax.fori_loop(0, count, fetch, 0)

    barrier = pltpu.get_barrier_semaphore()
    for neighbour in (left, right):
        pl.semaphore_signal(barrier, inc=1, device_id=neighbour, device_id_type=MESH)
    pl.semaphore_wait(barrier, 2)

    def gather_copy(j, way):
        d = j // 2
        c = lax.rem(j + way, 2)
        source = slot(d) if way == 0 else slot(n - d)
        return pltpu.make_async_remote_copy(
            src_ref=xbuf.at[source, part(c)],
            dst_ref=xbuf.at[source, part(c)],
            send_sem=send_sem.at[way, j],
            recv_sem=recv_sem.at[way, j],
            device_id=right if way == 0 else left,
            device_id_type=MESH,
        )

    def gather_arrival(j, way):
        d = j // 2 + 1
        c = lax.rem(j + way, 2)
        source = slot(d) if way == 0 else slot(n - d)
        return pltpu.make_async_remote_copy(
            src_ref=xbuf.at[source, part(c)],
            dst_ref=xbuf.at[source, part(c)],
            send_sem=send_sem.at[way, j],
            recv_sem=recv_sem.at[way, j],
            device_id=right if way == 0 else left,
            device_id_type=MESH,
        )

    own_copy = pltpu.make_async_copy(x_ref, xbuf.at[z], start_sem)
    own_copy.start()
    own_copy.wait()
    for j in range(2):
        for way in range(2):
            gather_copy(j, way).start()

    def pass_on(j):
        for way in range(2):
            gather_arrival(j, way).wait_recv()

        @pl.when(j + 2 < sent)
        def _():
            for way in range(2):
                gather_copy(j + 2, way).start()

    lanes = lax.broadcasted_iota(jnp.int32, (1, wt_ref.shape[2]), 1)
    main = ff // 128 * 128
    rest = ff - main
    cuts = [(a, min(a + 256, main)) for a in range(0, main, 256)]
    width = xbuf.shape[2]

    def gate_up(slots, k):
        x = jnp.concatenate([xbuf[s] for s in slots], axis=0) if len(slots) > 1 else xbuf[slots[0]]
        wrow = jnp.concatenate([wt_ref[s] for s in slots], axis=0) if len(slots) > 1 else wt_ref[slots[0]]
        scale = jnp.sum(jnp.where(lanes == k, wrow, 0.0), axis=1, keepdims=True)
        m = x.shape[0]

        def product(lo, hi):
            return jnp.dot(x, wi[k, :, lo:hi], preferred_element_type=jnp.float32)

        def put(lo, hi, g, u):
            a = g / (1.0 + jnp.exp(-g)) * u * scale
            act[k, 0:m, lo:hi] = a.astype(jnp.bfloat16)

        start = main + 2 * rest
        for lo, hi in cuts:
            if hi == main and rest:
                both = product(lo, start)
                put(lo, hi, both[:, :hi - lo], product(start + lo, start + hi))
                put(main, ff, both[:, hi - lo:hi - lo + rest], both[:, hi - lo + rest:])
            else:
                put(lo, hi, product(lo, hi), product(start + lo, start + hi))

    def down(slots):
        m = rows * len(slots)

        def columns(q, carry):
            span = pl.ds(pl.multiple_of(q * 512, min(512, width)), min(512, width))
            y = jnp.dot(act[0, 0:m, :], wd[0, :, span], preferred_element_type=jnp.float32)
            for k in range(1, count):
                y += jnp.dot(act[k, 0:m, :], wd[k, :, span], preferred_element_type=jnp.float32)
            y = y.astype(jnp.bfloat16)
            for i, s in enumerate(slots):
                acc[s, :, span] = y[i * rows:(i + 1) * rows]
            return carry

        lax.fori_loop(0, max(1, width // 512), columns, 0)

    def fetched(k, which):
        whole = (wi, wd)[which].at[k]
        pltpu.make_async_copy(whole, whole, wsem.at[k, which]).wait()

    def own_step(k, carry):
        fetched(k, 0)
        gate_up([z], k)

        @pl.when(k == 1)
        def _():
            pass_on(0)

        return carry

    lax.fori_loop(0, count, own_step, 0)
    for k in range(count):
        fetched(k, 1)
    down([z])

    def pair_step(p, carry):
        pass_on(2 * p - 1)
        slots = [slot(p), slot(n - p)]

        def one(k, inner):
            gate_up(slots, k)

            @pl.when(k == 1)
            def _():
                pass_on(2 * p)

            return inner

        lax.fori_loop(0, count, one, 0)
        down(slots)
        return carry

    lax.fori_loop(1, half_n, pair_step, 0)
    far = [slot(half_n)]

    def far_step(k, carry):
        gate_up(far, k)
        return carry

    lax.fori_loop(0, count, far_step, 0)
    down(far)
    for j in range(sent):
        for way in range(2):
            gather_copy(j, way).wait_send()

    bufs = (rbuf, lbuf)

    def sum_copy(j, way):
        return pltpu.make_async_remote_copy(
            src_ref=bufs[way].at[sent + j if j < 2 else j - 2],
            dst_ref=bufs[way].at[j],
            send_sem=send_sem.at[way, sent + j],
            recv_sem=recv_sem.at[way, sent + j],
            device_id=right if way == 0 else left,
            device_id_type=MESH,
        )

    for j in range(sent):
        for way in range(2):
            off = half_n - (j + 1) // 2
            owner = slot(n - off) if way == 0 else slot(off)
            c = (j + way) % 2
            own_part = acc[owner, part(c)]
            if j < 2:
                bufs[way][sent + j] = own_part
            else:
                sum_copy(j - 2, way).wait_recv()
                bufs[way][j - 2] = (bufs[way][j - 2].astype(jnp.float32) + own_part.astype(jnp.float32)).astype(jnp.bfloat16)
            sum_copy(j, way).start()
    for way in range(2):
        for j in (sent - 2, sent - 1):
            sum_copy(j, way).wait_recv()
    for c in range(2):
        total = hid_ref[part(c)] + acc[z, part(c)].astype(jnp.float32)
        for way in range(2):
            j = sent - 1 if (sent - 1 + way) % 2 == c else sent - 2
            total += bufs[way][j].astype(jnp.float32)
        out_ref[part(c)] = total.astype(jnp.bfloat16)
    for j in range(sent):
        for way in range(2):
            sum_copy(j, way).wait_send()


def mix_experts(normed, hidden, weight_table, inners, downs):
    rows, width = normed.shape
    n = lax.axis_size("z")
    pieces, count, depth, both = inners.shape
    ff = both // 2
    sent = n - 1
    vmem = pl.BlockSpec(memory_space=pltpu.VMEM)
    anywhere = pl.BlockSpec(memory_space=pl.ANY)
    return pl.pallas_call(
        functools.partial(moe_kernel, n),
        out_shape=jax.ShapeDtypeStruct((rows, width), jnp.bfloat16),
        in_specs=[vmem, vmem, vmem, anywhere, anywhere],
        out_specs=vmem,
        scratch_shapes=[
            pltpu.VMEM((n, rows, width), jnp.bfloat16),
            pltpu.VMEM((n, rows, width), jnp.bfloat16),
            pltpu.VMEM((count, 2 * rows, ff), jnp.bfloat16),
            pltpu.VMEM((count, pieces * depth, both), jnp.bfloat16),
            pltpu.VMEM((count, ff, pieces * depth), jnp.bfloat16),
            pltpu.VMEM((sent + 2, rows // 2, width), jnp.bfloat16),
            pltpu.VMEM((sent + 2, rows // 2, width), jnp.bfloat16),
            pltpu.SemaphoreType.DMA,
            pltpu.SemaphoreType.DMA((2, 2 * sent)),
            pltpu.SemaphoreType.DMA((2, 2 * sent)),
            pltpu.SemaphoreType.DMA((count, 2)),
        ],
        compiler_params=pltpu.CompilerParams(
            collective_id=0, has_side_effects=True, vmem_limit_bytes=66000000
        ),
        cost_estimate=pl.CostEstimate(
            flops=6 * n * rows * width * ff * count, bytes_accessed=40000000, transcendentals=0
        ),
    )(normed, hidden, weight_table, inners, downs)


def attend_items(query_items, key_items, value_items, segment_items):
    length, count_items, qk_width = query_items.shape
    block_rows = QUERY_BLOCK
    score_scale = qk_width ** (-0.5)
    key_positions = jnp.arange(length, dtype=jnp.int32)

    def one_block(block_index):
        first_row = block_index * block_rows
        query_block = lax.dynamic_slice_in_dim(query_items, first_row, block_rows, 0)
        scores = (
            jnp.einsum("qid,kid->iqk", query_block, key_items, preferred_element_type=jnp.float32)
            * score_scale
        )
        row_positions = first_row + jnp.arange(block_rows, dtype=jnp.int32)
        row_segments = lax.dynamic_slice_in_dim(segment_items, first_row, block_rows, 1)
        allowed = (row_positions[None, :, None] >= key_positions[None, None, :]) & (
            row_segments[:, :, None] == segment_items[:, None, :]
        )
        scores = jnp.where(allowed, scores, -jnp.inf)
        row_peak = jnp.max(scores, axis=2, keepdims=True)
        raised = jnp.exp(scores - row_peak)
        weights = (raised / jnp.sum(raised, axis=2, keepdims=True)).astype(jnp.bfloat16)
        return jnp.einsum(
            "iqk,kid->qid", weights, value_items, preferred_element_type=jnp.float32
        ).astype(jnp.bfloat16)

    blocks = lax.map(one_block, jnp.arange(length // block_rows, dtype=jnp.int32))
    return blocks.reshape(length, count_items, value_items.shape[2])


def column_weights(gate_matrix, up_matrix, down_matrix):
    parts = lax.axis_size(DP)
    depth = gate_matrix.shape[0] // parts
    first = lax.axis_index(DP) * depth
    gate_part = lax.dynamic_slice_in_dim(gate_matrix, first, depth, 0)
    up_part = lax.dynamic_slice_in_dim(up_matrix, first, depth, 0)
    main = gate_part.shape[1] // 128 * 128
    hidden_part = jnp.concatenate(
        [gate_part[:, :main], gate_part[:, main:], up_part[:, main:], up_part[:, :main]], axis=1
    )
    down_part = lax.dynamic_slice_in_dim(down_matrix, first, depth, 1)
    return [
        lax.all_gather(lax.all_gather(piece, "y"), DP) for piece in (hidden_part, down_part)
    ]


def column_table(routes, route_weights, expert_count):
    experts = jnp.arange(expert_count, dtype=jnp.int32)
    chosen = routes[:, :, None] == experts[None, None, :]
    table = jnp.sum(jnp.where(chosen, route_weights[:, :, None], 0.0), axis=1)
    table = lax.all_gather(table, "z")
    n = lax.axis_size("z")
    table = table.reshape(n, table.shape[1], expert_count // n, n)
    mine = jnp.arange(n, dtype=jnp.int32) == lax.axis_index("z")
    return jnp.sum(jnp.where(mine, table, 0.0), axis=3)


def body(
    queries,
    key_nope,
    key_rope,
    values,
    residual,
    segments,
    out_proj,
    norm_gain,
    expert_gate,
    expert_up,
    expert_down,
    routes,
    route_weights,
):
    half_rows, stream_count, query_width = queries.shape
    model_width = residual.shape[2]
    token_rows = half_rows * stream_count
    expert_count = lax.axis_size(EXPERT)
    item_count = stream_count * HEADS // expert_count
    inners, downs = column_weights(expert_gate[0], expert_up[0], expert_down[0])
    weight_table = column_table(routes[0, 0], route_weights[0, 0], expert_count)
    key_heads = jnp.concatenate(
        [
            key_nope.reshape(half_rows, stream_count, HEADS, NOPE),
            jnp.broadcast_to(key_rope[:, :, None, :], (half_rows, stream_count, HEADS, ROPE)),
        ],
        axis=3,
    )
    query_items = queries.reshape(half_rows, stream_count * HEADS, NOPE + ROPE)
    key_items = key_heads.reshape(half_rows, stream_count * HEADS, NOPE + ROPE)
    value_items = values.reshape(half_rows, stream_count * HEADS, V_DIM)
    query_all, key_all, value_all = side_by_side(
        (query_items, key_items, value_items), EXPERT, 1, 0, 2
    )
    item_ids = lax.axis_index(EXPERT) * item_count + jnp.arange(item_count, dtype=jnp.int32)
    stream_ids = item_ids // HEADS
    selector = (stream_ids[:, None] == jnp.arange(stream_count, dtype=jnp.int32)[None, :]).astype(
        jnp.int32
    )
    segment_items = jnp.sum(selector[:, :, None] * segments[None, :, :], axis=1)
    attended_items = attend_items(query_all, key_all, value_all, segment_items)
    attended_back = lax.all_to_all(
        attended_items, EXPERT, split_axis=0, concat_axis=1, tiled=True
    )
    attn_rows = attended_back.reshape(token_rows, HEADS * V_DIM)
    projected = jnp.dot(
        attn_rows,
        lax.all_gather(out_proj, DP + EXPERT, axis=0, tiled=True),
        preferred_element_type=jnp.float32,
    )
    hidden = residual.reshape(token_rows, model_width).astype(jnp.float32) + projected
    mean_square = jnp.mean(hidden * hidden, axis=1, keepdims=True)
    normed = (hidden * lax.rsqrt(mean_square + EPSILON) * norm_gain.astype(jnp.float32)).astype(
        jnp.bfloat16
    )
    layer_out = mix_experts(normed, hidden, weight_table, inners, downs)
    return layer_out.reshape(half_rows, stream_count, model_width)


def solution(mesh):
    split = Mesh(mesh.devices.reshape(4, 2, 4, 8), DP + EXPERT)
    rows = P(EXPERT, DP, None)
    weights = P(EXPERT, None, None)
    pairs = P(DP, EXPERT, None, None)
    return jax.shard_map(
        body,
        mesh=split,
        in_specs=(
            rows,
            rows,
            rows,
            rows,
            rows,
            P(DP, None),
            P(DP + EXPERT, None),
            P(),
            weights,
            weights,
            weights,
            pairs,
            pairs,
        ),
        out_specs=rows,
        check_vma=False,
    )
```

```python
import functools

import jax
import jax.numpy as jnp
from jax import lax
from jax.experimental import pallas as pl
from jax.experimental.pallas import tpu as pltpu
from jax.sharding import Mesh, PartitionSpec as P

MESH = pl.DeviceIdType.MESH
DP = ("x", "core")
EXPERT = ("y", "z")

HEADS = 16
NOPE = 128
ROPE = 64
V_DIM = 128
TOP = 6


EPSILON = 1e-06
QUERY_BLOCK = 512


def side_by_side(arrays, axis, split_dim, concat_dim, along):
    widths = [a.shape[along] for a in arrays]
    both = jnp.concatenate(arrays, axis=along)
    result = lax.all_to_all(both, axis, split_axis=split_dim, concat_axis=concat_dim, tiled=True)
    return tuple(jnp.split(result, [sum(widths[:k]) for k in range(1, len(widths))], axis=along))


def moe_kernel(axis_size, x_ref, hid_ref, wt_ref, own_g, own_u, own_d, *rest):
    pieces = rest[:24]
    (out_ref, xbuf, acc, act, weights, rbuf, lbuf, start_sem, send_sem, recv_sem, wsem) = rest[24:]
    n = axis_size
    half_n = n // 2
    z = lax.axis_index("z")
    right = {"z": lax.rem(z + 1, n)}
    left = {"z": lax.rem(z + n - 1, n)}
    rows = x_ref.shape[0]
    half = rows // 2
    count, _, ff, width = weights.shape
    high, wide = pieces[0].shape[1:]
    sent = 2 * half_n - 1

    def slot(d):
        return lax.rem(z + 2 * n - d, n)

    def part(c):
        return pl.ds(pl.multiple_of(c * half, half), half)

    for i, own in enumerate((own_g, own_u, own_d)):
        pltpu.make_async_copy(own, weights.at[0, i], wsem.at[0]).start()
    core = lax.axis_index("core")
    for i, piece in enumerate(pieces):
        k, quarter, half_of = 1 + i // 8, i % 8 // 2, i % 2
        column = pl.multiple_of(lax.rem(core + half_of, 2) * wide, wide)
        target = weights.at[k, :, pl.ds(quarter * high, high), pl.ds(column, wide)]
        pltpu.make_async_copy(piece, target, wsem.at[k]).start()

    barrier = pltpu.get_barrier_semaphore()
    for neighbour in (left, right):
        pl.semaphore_signal(barrier, inc=1, device_id=neighbour, device_id_type=MESH)
    pl.semaphore_wait(barrier, 2)

    def gather_copy(j, way):
        d = j // 2
        c = lax.rem(j + way, 2)
        source = slot(d) if way == 0 else slot(n - d)
        return pltpu.make_async_remote_copy(
            src_ref=xbuf.at[source, part(c)],
            dst_ref=xbuf.at[source, part(c)],
            send_sem=send_sem.at[way, j],
            recv_sem=recv_sem.at[way, j],
            device_id=right if way == 0 else left,
            device_id_type=MESH,
        )

    def gather_arrival(j, way):
        d = j // 2 + 1
        c = lax.rem(j + way, 2)
        source = slot(d) if way == 0 else slot(n - d)
        return pltpu.make_async_remote_copy(
            src_ref=xbuf.at[source, part(c)],
            dst_ref=xbuf.at[source, part(c)],
            send_sem=send_sem.at[way, j],
            recv_sem=recv_sem.at[way, j],
            device_id=right if way == 0 else left,
            device_id_type=MESH,
        )

    own_copy = pltpu.make_async_copy(x_ref, xbuf.at[z], start_sem)
    own_copy.start()
    own_copy.wait()
    for j in range(2):
        for way in range(2):
            gather_copy(j, way).start()

    def pass_on(j):
        for way in range(2):
            gather_arrival(j, way).wait_recv()

        @pl.when(j + 2 < sent)
        def _():
            for way in range(2):
                gather_copy(j + 2, way).start()

    lanes = lax.broadcasted_iota(jnp.int32, (1, wt_ref.shape[2]), 1)
    cuts = [(a, min(a + 256, ff)) for a in range(0, ff, 256)]

    def gate_up(slots, k):
        x = jnp.concatenate([xbuf[s] for s in slots], axis=0) if len(slots) > 1 else xbuf[slots[0]]
        wrow = jnp.concatenate([wt_ref[s] for s in slots], axis=0) if len(slots) > 1 else wt_ref[slots[0]]
        scale = jnp.sum(jnp.where(lanes == k, wrow, 0.0), axis=1, keepdims=True)
        m = x.shape[0]

        def product(which, lo, hi):
            return lax.dot_general(
                x, weights[k, which, lo:hi], (((1,), (1,)), ((), ())), preferred_element_type=jnp.float32
            )

        for lo, hi in cuts:
            g, u = product(0, lo, hi), product(1, lo, hi)
            a = g / (1.0 + jnp.exp(-g)) * u * scale
            act[k, 0:m, lo:hi] = a.astype(jnp.bfloat16)

    def down(slots):
        m = rows * len(slots)

        def columns(q, carry):
            span = pl.ds(pl.multiple_of(q * 512, min(512, width)), min(512, width))
            y = jnp.dot(act[0, 0:m, :], weights[0, 2, :, span], preferred_element_type=jnp.float32)
            for k in range(1, count):
                y += jnp.dot(act[k, 0:m, :], weights[k, 2, :, span], preferred_element_type=jnp.float32)
            y = y.astype(jnp.bfloat16)
            for i, s in enumerate(slots):
                acc[s, :, span] = y[i * rows:(i + 1) * rows]
            return carry

        lax.fori_loop(0, max(1, width // 512), columns, 0)

    def fetched(k):
        whole = weights.at[k]
        pltpu.make_async_copy(whole, whole, wsem.at[k]).wait()

    def own_step(k, carry):
        fetched(k)
        gate_up([z], k)

        @pl.when(k == 1)
        def _():
            pass_on(0)

        return carry

    lax.fori_loop(0, count, own_step, 0)
    down([z])

    def pair_step(p, carry):
        pass_on(2 * p - 1)
        slots = [slot(p), slot(n - p)]

        def one(k, inner):
            gate_up(slots, k)

            @pl.when(k == 1)
            def _():
                pass_on(2 * p)

            return inner

        lax.fori_loop(0, count, one, 0)
        down(slots)
        return carry

    lax.fori_loop(1, half_n, pair_step, 0)
    far = [slot(half_n)]

    def far_step(k, carry):
        gate_up(far, k)
        return carry

    lax.fori_loop(0, count, far_step, 0)
    down(far)
    for j in range(sent):
        for way in range(2):
            gather_copy(j, way).wait_send()

    bufs = (rbuf, lbuf)

    def sum_copy(j, way):
        return pltpu.make_async_remote_copy(
            src_ref=bufs[way].at[sent + j if j < 2 else j - 2],
            dst_ref=bufs[way].at[j],
            send_sem=send_sem.at[way, sent + j],
            recv_sem=recv_sem.at[way, sent + j],
            device_id=right if way == 0 else left,
            device_id_type=MESH,
        )

    for j in range(sent):
        for way in range(2):
            off = half_n - (j + 1) // 2
            owner = slot(n - off) if way == 0 else slot(off)
            c = (j + way) % 2
            own_part = acc[owner, part(c)]
            if j < 2:
                bufs[way][sent + j] = own_part
            else:
                sum_copy(j - 2, way).wait_recv()
                bufs[way][j - 2] = (bufs[way][j - 2].astype(jnp.float32) + own_part.astype(jnp.float32)).astype(jnp.bfloat16)
            sum_copy(j, way).start()
    for way in range(2):
        for j in (sent - 2, sent - 1):
            sum_copy(j, way).wait_recv()
    for c in range(2):
        total = hid_ref[part(c)] + acc[z, part(c)].astype(jnp.float32)
        for way in range(2):
            j = sent - 1 if (sent - 1 + way) % 2 == c else sent - 2
            total += bufs[way][j].astype(jnp.float32)
        out_ref[part(c)] = total.astype(jnp.bfloat16)
    for j in range(sent):
        for way in range(2):
            sum_copy(j, way).wait_send()


def mix_experts(normed, hidden, weight_table, own_weights, other_weights):
    rows, width = normed.shape
    n = lax.axis_size("z")
    ff = own_weights[2].shape[0]
    count = 1 + len(other_weights)
    pieces = [half for source in other_weights for quarter in source for half in quarter]
    sent = n - 1
    vmem = pl.BlockSpec(memory_space=pltpu.VMEM)
    anywhere = pl.BlockSpec(memory_space=pl.ANY)
    return pl.pallas_call(
        functools.partial(moe_kernel, n),
        out_shape=jax.ShapeDtypeStruct((rows, width), jnp.bfloat16),
        in_specs=[vmem] * 3 + [anywhere] * (3 + len(pieces)),
        out_specs=vmem,
        scratch_shapes=[
            pltpu.VMEM((n, rows, width), jnp.bfloat16),
            pltpu.VMEM((n, rows, width), jnp.bfloat16),
            pltpu.VMEM((count, 2 * rows, ff), jnp.bfloat16),
            pltpu.VMEM((count, 3, ff, width), jnp.bfloat16),
            pltpu.VMEM((sent + 2, rows // 2, width), jnp.bfloat16),
            pltpu.VMEM((sent + 2, rows // 2, width), jnp.bfloat16),
            pltpu.SemaphoreType.DMA,
            pltpu.SemaphoreType.DMA((2, 2 * sent)),
            pltpu.SemaphoreType.DMA((2, 2 * sent)),
            pltpu.SemaphoreType.DMA((count,)),
        ],
        compiler_params=pltpu.CompilerParams(
            collective_id=0, has_side_effects=True, vmem_limit_bytes=66000000
        ),
        cost_estimate=pl.CostEstimate(
            flops=6 * n * rows * width * ff * count, bytes_accessed=40000000, transcendentals=0
        ),
    )(normed, hidden, weight_table, *own_weights, *pieces)


def attend_items(query_items, key_items, value_items, segment_items):
    length, count_items, qk_width = query_items.shape
    block_rows = QUERY_BLOCK
    score_scale = qk_width ** (-0.5)
    key_positions = jnp.arange(length, dtype=jnp.int32)

    def one_block(block_index):
        first_row = block_index * block_rows
        query_block = lax.dynamic_slice_in_dim(query_items, first_row, block_rows, 0)
        scores = (
            jnp.einsum("qid,kid->iqk", query_block, key_items, preferred_element_type=jnp.float32)
            * score_scale
        )
        row_positions = first_row + jnp.arange(block_rows, dtype=jnp.int32)
        row_segments = lax.dynamic_slice_in_dim(segment_items, first_row, block_rows, 1)
        allowed = (row_positions[None, :, None] >= key_positions[None, None, :]) & (
            row_segments[:, :, None] == segment_items[:, None, :]
        )
        scores = jnp.where(allowed, scores, -jnp.inf)
        row_peak = jnp.max(scores, axis=2, keepdims=True)
        raised = jnp.exp(scores - row_peak)
        weights = (raised / jnp.sum(raised, axis=2, keepdims=True)).astype(jnp.bfloat16)
        return jnp.einsum(
            "iqk,kid->qid", weights, value_items, preferred_element_type=jnp.float32
        ).astype(jnp.bfloat16)

    blocks = lax.map(one_block, jnp.arange(length // block_rows, dtype=jnp.int32))
    return blocks.reshape(length, count_items, value_items.shape[2])


def column_weights(gate_matrix, up_matrix, down_matrix):
    size_x, size_y = lax.axis_size("x"), lax.axis_size("y")
    ff, width = down_matrix.shape
    high, wide = ff // size_x, width // 2
    mine, core = lax.axis_index("x"), lax.axis_index("core")

    def piece(quarter):
        first = (lax.rem(quarter, size_x) * high, core * wide)
        return jnp.stack(
            [lax.dynamic_slice(w, first, (high, wide)) for w in (gate_matrix, up_matrix, down_matrix)]
        )

    def shift(array, axis, by):
        n = lax.axis_size(axis)
        return lax.ppermute(array, axis, [(i, (i + by) % n) for i in range(n)])

    one, two = piece(mine), piece(mine + 1)
    left = [shift(one, "y", 1), shift(two, "y", 1)]
    right = [shift(one, "y", -1), shift(two, "y", -1)]
    far = [shift(left[0], "y", 1), shift(right[1], "y", -1)]
    result = []
    for source in (left, right, far):
        quarters = source + [shift(source[1], "x", -1), shift(source[0], "x", 1)]
        result.append([(quarter, shift(quarter, "core", 1)) for quarter in quarters])
    return result


def column_table(routes, route_weights, expert_count):
    experts = jnp.arange(expert_count, dtype=jnp.int32)
    chosen = routes[:, :, None] == experts[None, None, :]
    table = jnp.sum(jnp.where(chosen, route_weights[:, :, None], 0.0), axis=1)
    table = lax.all_gather(table, "z")
    n = lax.axis_size("z")
    table = table.reshape(n, table.shape[1], expert_count // n, n)
    mine = jnp.arange(n, dtype=jnp.int32) == lax.axis_index("z")
    table = jnp.sum(jnp.where(mine, table, 0.0), axis=3)
    count = expert_count // n
    order = lax.rem(lax.axis_index("y") + jnp.array([0, count - 1, 1, 2], jnp.int32), count)
    picks = order[:, None] == jnp.arange(count, dtype=jnp.int32)[None, :]
    return jnp.sum(jnp.where(picks, table[:, :, None, :], 0.0), axis=3)


def body(
    queries,
    key_nope,
    key_rope,
    values,
    residual,
    segments,
    out_proj,
    norm_gain,
    expert_gate,
    expert_up,
    expert_down,
    routes,
    route_weights,
):
    half_rows, stream_count, query_width = queries.shape
    model_width = residual.shape[2]
    token_rows = half_rows * stream_count
    expert_count = lax.axis_size(EXPERT)
    item_count = stream_count * HEADS // expert_count
    own_weights = (expert_gate[0].T, expert_up[0].T, expert_down[0])
    other_weights = column_weights(*own_weights)
    weight_table = column_table(routes[0, 0], route_weights[0, 0], expert_count)
    key_heads = jnp.concatenate(
        [
            key_nope.reshape(half_rows, stream_count, HEADS, NOPE),
            jnp.broadcast_to(key_rope[:, :, None, :], (half_rows, stream_count, HEADS, ROPE)),
        ],
        axis=3,
    )
    query_items = queries.reshape(half_rows, stream_count * HEADS, NOPE + ROPE)
    key_items = key_heads.reshape(half_rows, stream_count * HEADS, NOPE + ROPE)
    value_items = values.reshape(half_rows, stream_count * HEADS, V_DIM)
    query_all, key_all, value_all = side_by_side(
        (query_items, key_items, value_items), EXPERT, 1, 0, 2
    )
    item_ids = lax.axis_index(EXPERT) * item_count + jnp.arange(item_count, dtype=jnp.int32)
    stream_ids = item_ids // HEADS
    selector = (stream_ids[:, None] == jnp.arange(stream_count, dtype=jnp.int32)[None, :]).astype(
        jnp.int32
    )
    segment_items = jnp.sum(selector[:, :, None] * segments[None, :, :], axis=1)
    attended_items = attend_items(query_all, key_all, value_all, segment_items)
    attended_back = lax.all_to_all(
        attended_items, EXPERT, split_axis=0, concat_axis=1, tiled=True
    )
    attn_rows = attended_back.reshape(token_rows, HEADS * V_DIM)
    projected = jnp.dot(
        attn_rows,
        lax.all_gather(out_proj, DP + EXPERT, axis=0, tiled=True),
        preferred_element_type=jnp.float32,
    )
    hidden = residual.reshape(token_rows, model_width).astype(jnp.float32) + projected
    mean_square = jnp.mean(hidden * hidden, axis=1, keepdims=True)
    normed = (hidden * lax.rsqrt(mean_square + EPSILON) * norm_gain.astype(jnp.float32)).astype(
        jnp.bfloat16
    )
    layer_out = mix_experts(normed, hidden, weight_table, own_weights, other_weights)
    return layer_out.reshape(half_rows, stream_count, model_width)


def solution(mesh):
    split = Mesh(mesh.devices.reshape(4, 2, 4, 8), DP + EXPERT)
    rows = P(EXPERT, DP, None)
    weights = P(EXPERT, None, None)
    pairs = P(DP, EXPERT, None, None)
    return jax.shard_map(
        body,
        mesh=split,
        in_specs=(
            rows,
            rows,
            rows,
            rows,
            rows,
            P(DP, None),
            P(DP + EXPERT, None),
            P(),
            weights,
            weights,
            weights,
            pairs,
            pairs,
        ),
        out_specs=rows,
        check_vma=False,
    )
```

```python
import functools

import jax
import jax.numpy as jnp
from jax import lax
from jax.experimental import pallas as pl
from jax.experimental.pallas import tpu as pltpu
from jax.sharding import Mesh, PartitionSpec as P

MESH = pl.DeviceIdType.MESH
DP = ("x", "core")
EXPERT = ("y", "z")

HEADS = 16
NOPE = 128
ROPE = 64
V_DIM = 128
TOP = 6


EPSILON = 1e-06
QUERY_BLOCK = 512


def front_kernel(qkv, bound, table, own_g, own_u, own_d, attn_ref, tab_ref, others,
                 rows_buf, qbuf, kbuf, att, local_sem, a2a_sem, att_sem, tab_sem,
                 ysend, yrecv, fsend, frecv, xsend, xrecv, csend, crecv):
    size_x, size_y, size_z = lax.axis_size("x"), lax.axis_size("y"), lax.axis_size("z")
    peers = size_y * size_z
    x, core = lax.axis_index("x"), lax.axis_index("core")
    y, z = lax.axis_index("y"), lax.axis_index("z")
    me = y * size_z + z
    up_y, down_y = {"y": lax.rem(y + 1, size_y)}, {"y": lax.rem(y + size_y - 1, size_y)}
    up_x, down_x = {"x": lax.rem(x + 1, size_x)}, {"x": lax.rem(x + size_x - 1, size_x)}
    other_core = {"core": 1 - core}
    block = qkv.shape[1]
    heads = attn_ref.shape[1] // V_DIM
    ff, width = own_d.shape
    high, wide = ff // size_x, width // 4

    def peer(e):
        return {"y": lax.div(e, size_z), "z": lax.rem(e, size_z)}

    def remote(src, dst, send, recv, device):
        return pltpu.make_async_remote_copy(
            src_ref=src, dst_ref=dst, send_sem=send, recv_sem=recv, device_id=device, device_id_type=MESH
        )

    barrier = pltpu.get_barrier_semaphore()

    def greet(d, carry):
        pl.semaphore_signal(barrier, inc=1, device_id=peer(lax.rem(me + d, peers)), device_id_type=MESH)
        return carry

    lax.fori_loop(1, peers, greet, 0)
    for device in (up_x, down_x, other_core):
        pl.semaphore_signal(barrier, inc=1, device_id=device, device_id_type=MESH)
    pl.semaphore_wait(barrier, peers + 2)

    def rows_of(e):
        return pl.ds(pl.multiple_of(e * block, block), block)

    def send_rows(d, carry):
        e = lax.rem(me + d, peers)
        remote(qkv.at[e], rows_buf.at[rows_of(me)], a2a_sem.at[0], a2a_sem.at[1], peer(e)).start()
        return carry

    lax.fori_loop(1, peers, send_rows, 0)
    own_rows = pltpu.make_async_copy(qkv.at[me], rows_buf.at[rows_of(me)], local_sem.at[0])
    own_rows.start()

    def columns(u):
        return pl.ds(pl.multiple_of((core * 2 + u) * wide, wide), wide)

    def region(s, q, u):
        return others.at[s, :, pl.ds(q * high, high), columns(u)]

    def y_index(s, q, u):
        return (s * 2 + q) * 2 + u

    def y_start(s, q, u):
        n = y_index(s, q, u)
        quarter = pl.ds(pl.multiple_of(lax.rem(x + q, size_x) * high, high), high)
        for m, own in enumerate((own_g, own_u, own_d)):
            remote(
                own.at[quarter, columns(u)],
                others.at[s, m, pl.ds(q * high, high), columns(u)],
                ysend.at[n],
                yrecv.at[n],
                up_y if s == 0 else down_y,
            ).start()

    def y_copy(s, q, u):
        n = y_index(s, q, u)
        return remote(region(s, q, u), region(s, q, u), ysend.at[n], yrecv.at[n], up_y)

    def f_copy(q, u):
        source, device = (0, up_y) if q == 0 else (1, down_y)
        n = q * 2 + u
        return remote(region(source, q, u), region(2, q, u), fsend.at[n], frecv.at[n], device)

    def x_copy(s, q, u):
        device, slot = (up_x, 3) if q == 0 else (down_x, 2)
        n = (s * 2 + q) * 2 + u
        return remote(region(s, q, u), region(s, slot, u), xsend.at[n], xrecv.at[n], device)

    def c_copy(s, q, u):
        n = (s * 4 + q) * 2 + u
        return remote(region(s, q, u), region(s, q, u), csend.at[n], crecv.at[n], other_core)

    for first in (True, False):
        for u in range(2):
            for s in range(2):
                y_start(s, s if first else 1 - s, u)

    def tab_copy(d):
        to = lax.rem(z + d, size_z)
        return remote(table.at[to], tab_ref.at[z], tab_sem.at[0], tab_sem.at[1], {"z": to})

    for d in range(1, size_z):
        tab_copy(d).start()
    own_table = pltpu.make_async_copy(table.at[z], tab_ref.at[z], local_sem.at[1])
    own_table.start()

    def arrived(s, q, u):
        x_copy(s, q, u).start()
        c_copy(s, q, u).start()

    for u in range(2):
        for s in range(2):
            y_copy(s, s, u).wait_recv()
            f_copy(s, u).start()
            arrived(s, s, u)

    own_rows.wait()
    most = rows_buf.at[pl.ds(0, (peers - 1) * block)]
    remote(most, most, a2a_sem.at[0], a2a_sem.at[1], up_y).wait_recv()

    length = rows_buf.shape[0]
    lane = lax.broadcasted_iota(jnp.int32, (1, 128), 1)
    swap = (
        lax.broadcasted_iota(jnp.int32, (128, 128), 0) == lax.broadcasted_iota(jnp.int32, (128, 128), 1) + ROPE
    ).astype(jnp.bfloat16)

    step = min(512, length)
    strip = min(256, step)

    def arrange(i, carry):
        span = pl.ds(pl.multiple_of(i * step, step), step)
        rope = rows_buf[span, 384:512]
        qbuf[span, 0:128] = rows_buf[span, 0:128]
        qbuf[span, 128:256] = jnp.where(lane < ROPE, rope, jnp.zeros_like(rope))
        kbuf[span, 0:128] = rows_buf[span, 128:256]
        kbuf[span, 128:256] = jnp.dot(rope, swap, preferred_element_type=jnp.float32).astype(jnp.bfloat16)
        return carry

    lax.fori_loop(0, length // step, arrange, 0)
    border = bound[0]
    scale = (NOPE + ROPE) ** (-0.5)
    stream, head = lax.div(me, heads), lax.rem(me, heads)
    target = (
        pl.ds(pl.multiple_of(stream * block, block), block),
        pl.ds(pl.multiple_of(head * V_DIM, V_DIM), V_DIM),
    )

    def back_copy(e):
        return remote(att.at[rows_of(e)], attn_ref.at[target[0], target[1]], att_sem.at[0], att_sem.at[1], peer(e))

    def local_back():
        return pltpu.make_async_copy(att.at[rows_of(me)], attn_ref.at[target[0], target[1]], local_sem.at[2])

    def attend(i):
        limit = (i + 1) * step

        def one(j, carry):
            first = i * step + j * strip
            span = pl.ds(pl.multiple_of(first, strip), strip)
            scores = lax.dot_general(
                qbuf[span, :], kbuf[0:limit, :], (((1,), (1,)), ((), ())), preferred_element_type=jnp.float32
            ) * scale
            row = first + lax.broadcasted_iota(jnp.int32, (strip, 1), 0)
            column = lax.broadcasted_iota(jnp.int32, (1, limit), 1)
            lowest = jnp.where(row >= border, border, 0)
            scores = jnp.where((column <= row) & (column >= lowest), scores, -jnp.inf)
            raised = jnp.exp(scores - jnp.max(scores, axis=1, keepdims=True))
            total = jnp.sum(raised, axis=1, keepdims=True)
            mixed = jnp.dot(
                raised.astype(jnp.bfloat16), rows_buf[0:limit, 256:384], preferred_element_type=jnp.float32
            )
            att[span, :] = (mixed / total).astype(jnp.bfloat16)
            for t in range(strip // block):
                e = lax.div(first, block) + t

                @pl.when(e != me)
                def _():
                    back_copy(e).start()

                @pl.when(e == me)
                def _():
                    local_back().start()

            return carry

        lax.fori_loop(0, step // strip, one, 0)

    count = length // step
    for i in range(count):
        attend(i)
        if i == count // 2 - 1:
            for u in range(2):
                for s in range(2):
                    y_copy(s, 1 - s, u).wait_recv()
                    arrived(s, 1 - s, u)

    def crossed(s, q, u):
        x_copy(s, q, u).wait_recv()
        c_copy(s, 3 if q == 0 else 2, u).start()

    for u in range(2):
        for s in range(2):
            crossed(s, s, u)
    for u in range(2):
        for q in range(2):
            f_copy(q, u).wait_recv()
            arrived(2, q, u)
    for u in range(2):
        for s in range(2):
            crossed(s, 1 - s, u)
    for u in range(2):
        for q in range(2):
            crossed(2, q, u)

    for s in range(3):
        for q in range(4):
            for u in range(2):
                c_copy(s, q, u).wait()
    for u in range(2):
        for q in range(2):
            for s in range(2):
                y_copy(s, q, u).wait_send()
            f_copy(q, u).wait_send()
            for s in range(3):
                x_copy(s, q, u).wait_send()
    remote(most, most, a2a_sem.at[0], a2a_sem.at[1], up_y).wait_send()
    local_back().wait()
    back = att.at[pl.ds(0, (peers - 1) * block)]
    remote(back, back, att_sem.at[0], att_sem.at[1], up_y).wait()
    own_table.wait()
    tables = tab_ref.at[pl.ds(0, size_z - 1)]
    remote(tables, tables, tab_sem.at[0], tab_sem.at[1], up_y).wait()


def attend_and_gather(qkv, bound, table, own_weights):
    peers, block, packed = qkv.shape
    ff, width = own_weights[2].shape
    heads = width // V_DIM
    length = peers * block
    vmem = pl.BlockSpec(memory_space=pltpu.VMEM)
    anywhere = pl.BlockSpec(memory_space=pl.ANY)
    dma = pltpu.SemaphoreType.DMA
    return pl.pallas_call(
        front_kernel,
        out_shape=(
            jax.ShapeDtypeStruct((peers // heads * block, width), jnp.bfloat16),
            jax.ShapeDtypeStruct(table.shape, jnp.float32),
            jax.ShapeDtypeStruct((3, 3, ff, width), jnp.bfloat16),
        ),
        in_specs=[anywhere, pl.BlockSpec(memory_space=pltpu.SMEM), vmem] + [anywhere] * 3,
        out_specs=(vmem, vmem, anywhere),
        scratch_shapes=[
            pltpu.VMEM((length, packed), jnp.bfloat16),
            pltpu.VMEM((length, 256), jnp.bfloat16),
            pltpu.VMEM((length, 256), jnp.bfloat16),
            pltpu.VMEM((length, V_DIM), jnp.bfloat16),
            dma((3,)),
            dma((2,)),
            dma((2,)),
            dma((2,)),
            dma((8,)),
            dma((8,)),
            dma((4,)),
            dma((4,)),
            dma((12,)),
            dma((12,)),
            dma((24,)),
            dma((24,)),
        ],
        compiler_params=pltpu.CompilerParams(
            collective_id=1, has_side_effects=True, vmem_limit_bytes=50000000
        ),
        cost_estimate=pl.CostEstimate(flops=100000000000, bytes_accessed=40000000, transcendentals=0),
    )(qkv, bound, table, *own_weights)


def moe_kernel(axis_size, x_ref, hid_ref, wt_ref, own_g, own_u, own_d, others,
               out_ref, xbuf, acc, act, weights, rbuf, lbuf, start_sem, send_sem, recv_sem, wsem):
    n = axis_size
    half_n = n // 2
    y, z = lax.axis_index("y"), lax.axis_index("z")
    right = {"z": lax.rem(z + 1, n)}
    left = {"z": lax.rem(z + n - 1, n)}
    rows = x_ref.shape[0]
    half = rows // 2
    count, _, ff, width = weights.shape
    sent = 2 * half_n - 1

    def slot(d):
        return lax.rem(z + 2 * n - d, n)

    def part(c):
        return pl.ds(pl.multiple_of(c * half, half), half)

    for i, own in enumerate((own_g, own_u, own_d)):
        pltpu.make_async_copy(own, weights.at[0, i], wsem.at[0]).start()
    for k in range(1, count):
        pltpu.make_async_copy(others.at[k - 1], weights.at[k], wsem.at[k]).start()

    barrier = pltpu.get_barrier_semaphore()
    for neighbour in (left, right):
        pl.semaphore_signal(barrier, inc=1, device_id=neighbour, device_id_type=MESH)
    pl.semaphore_wait(barrier, 2)

    def gather_copy(j, way):
        d = j // 2
        c = lax.rem(j + way, 2)
        source = slot(d) if way == 0 else slot(n - d)
        return pltpu.make_async_remote_copy(
            src_ref=xbuf.at[source, part(c)],
            dst_ref=xbuf.at[source, part(c)],
            send_sem=send_sem.at[way, j],
            recv_sem=recv_sem.at[way, j],
            device_id=right if way == 0 else left,
            device_id_type=MESH,
        )

    def gather_arrival(j, way):
        d = j // 2 + 1
        c = lax.rem(j + way, 2)
        source = slot(d) if way == 0 else slot(n - d)
        return pltpu.make_async_remote_copy(
            src_ref=xbuf.at[source, part(c)],
            dst_ref=xbuf.at[source, part(c)],
            send_sem=send_sem.at[way, j],
            recv_sem=recv_sem.at[way, j],
            device_id=right if way == 0 else left,
            device_id_type=MESH,
        )

    own_copy = pltpu.make_async_copy(x_ref, xbuf.at[z], start_sem)
    own_copy.start()
    own_copy.wait()
    for j in range(2):
        for way in range(2):
            gather_copy(j, way).start()

    def pass_on(j):
        for way in range(2):
            gather_arrival(j, way).wait_recv()

        @pl.when(j + 2 < sent)
        def _():
            for way in range(2):
                gather_copy(j + 2, way).start()

    lanes = lax.broadcasted_iota(jnp.int32, (1, wt_ref.shape[2]), 1)
    cuts = [(a, min(a + 256, ff)) for a in range(0, ff, 256)]

    def gate_up(slots, k):
        x = jnp.concatenate([xbuf[s] for s in slots], axis=0) if len(slots) > 1 else xbuf[slots[0]]
        wrow = jnp.concatenate([wt_ref[s] for s in slots], axis=0) if len(slots) > 1 else wt_ref[slots[0]]
        offset = jnp.where(k == 0, 0, jnp.where(k == 1, count - 1, k - 1))
        scale = jnp.sum(jnp.where(lanes == lax.rem(y + offset, count), wrow, 0.0), axis=1, keepdims=True)
        m = x.shape[0]

        def product(which, lo, hi):
            return lax.dot_general(
                x, weights[k, which, lo:hi], (((1,), (1,)), ((), ())), preferred_element_type=jnp.float32
            )

        for lo, hi in cuts:
            g, u = product(0, lo, hi), product(1, lo, hi)
            a = g / (1.0 + jnp.exp(-g)) * u * scale
            act[k, 0:m, lo:hi] = a.astype(jnp.bfloat16)

    def down(slots):
        m = rows * len(slots)

        def columns(q, carry):
            span = pl.ds(pl.multiple_of(q * 512, min(512, width)), min(512, width))
            y = jnp.dot(act[0, 0:m, :], weights[0, 2, :, span], preferred_element_type=jnp.float32)
            for k in range(1, count):
                y += jnp.dot(act[k, 0:m, :], weights[k, 2, :, span], preferred_element_type=jnp.float32)
            y = y.astype(jnp.bfloat16)
            for i, s in enumerate(slots):
                acc[s, :, span] = y[i * rows:(i + 1) * rows]
            return carry

        lax.fori_loop(0, max(1, width // 512), columns, 0)

    def fetched(k):
        whole = weights.at[k]
        pltpu.make_async_copy(whole, whole, wsem.at[k]).wait()

    def own_step(k, carry):
        fetched(k)
        gate_up([z], k)

        @pl.when(k == 1)
        def _():
            pass_on(0)

        return carry

    lax.fori_loop(0, count, own_step, 0)
    down([z])

    def pair_step(p, carry):
        pass_on(2 * p - 1)
        slots = [slot(p), slot(n - p)]

        def one(k, inner):
            gate_up(slots, k)

            @pl.when(k == 1)
            def _():
                pass_on(2 * p)

            return inner

        lax.fori_loop(0, count, one, 0)
        down(slots)
        return carry

    lax.fori_loop(1, half_n, pair_step, 0)
    far = [slot(half_n)]

    def far_step(k, carry):
        gate_up(far, k)
        return carry

    lax.fori_loop(0, count, far_step, 0)
    down(far)
    for j in range(sent):
        for way in range(2):
            gather_copy(j, way).wait_send()

    bufs = (rbuf, lbuf)

    def sum_copy(j, way):
        return pltpu.make_async_remote_copy(
            src_ref=bufs[way].at[sent + j if j < 2 else j - 2],
            dst_ref=bufs[way].at[j],
            send_sem=send_sem.at[way, sent + j],
            recv_sem=recv_sem.at[way, sent + j],
            device_id=right if way == 0 else left,
            device_id_type=MESH,
        )

    for j in range(sent):
        for way in range(2):
            off = half_n - (j + 1) // 2
            owner = slot(n - off) if way == 0 else slot(off)
            c = (j + way) % 2
            own_part = acc[owner, part(c)]
            if j < 2:
                bufs[way][sent + j] = own_part
            else:
                sum_copy(j - 2, way).wait_recv()
                bufs[way][j - 2] = (bufs[way][j - 2].astype(jnp.float32) + own_part.astype(jnp.float32)).astype(jnp.bfloat16)
            sum_copy(j, way).start()
    for way in range(2):
        for j in (sent - 2, sent - 1):
            sum_copy(j, way).wait_recv()
    for c in range(2):
        total = hid_ref[part(c)] + acc[z, part(c)].astype(jnp.float32)
        for way in range(2):
            j = sent - 1 if (sent - 1 + way) % 2 == c else sent - 2
            total += bufs[way][j].astype(jnp.float32)
        out_ref[part(c)] = total.astype(jnp.bfloat16)
    for j in range(sent):
        for way in range(2):
            sum_copy(j, way).wait_send()


def mix_experts(normed, hidden, weight_table, own_weights, other_weights):
    rows, width = normed.shape
    n = lax.axis_size("z")
    ff = own_weights[2].shape[0]
    count = 1 + other_weights.shape[0]
    sent = n - 1
    vmem = pl.BlockSpec(memory_space=pltpu.VMEM)
    anywhere = pl.BlockSpec(memory_space=pl.ANY)
    return pl.pallas_call(
        functools.partial(moe_kernel, n),
        out_shape=jax.ShapeDtypeStruct((rows, width), jnp.bfloat16),
        in_specs=[vmem] * 3 + [anywhere] * 4,
        out_specs=vmem,
        scratch_shapes=[
            pltpu.VMEM((n, rows, width), jnp.bfloat16),
            pltpu.VMEM((n, rows, width), jnp.bfloat16),
            pltpu.VMEM((count, 2 * rows, ff), jnp.bfloat16),
            pltpu.VMEM((count, 3, ff, width), jnp.bfloat16),
            pltpu.VMEM((sent + 2, rows // 2, width), jnp.bfloat16),
            pltpu.VMEM((sent + 2, rows // 2, width), jnp.bfloat16),
            pltpu.SemaphoreType.DMA,
            pltpu.SemaphoreType.DMA((2, 2 * sent)),
            pltpu.SemaphoreType.DMA((2, 2 * sent)),
            pltpu.SemaphoreType.DMA((count,)),
        ],
        compiler_params=pltpu.CompilerParams(
            collective_id=0, has_side_effects=True, vmem_limit_bytes=66000000
        ),
        cost_estimate=pl.CostEstimate(
            flops=6 * n * rows * width * ff * count, bytes_accessed=40000000, transcendentals=0
        ),
    )(normed, hidden, weight_table, *own_weights, other_weights)


def column_table(routes, route_weights, expert_count, n):
    experts = jnp.arange(expert_count, dtype=jnp.int32)
    chosen = routes[:, :, None] == experts[None, None, :]
    table = jnp.sum(jnp.where(chosen, route_weights[:, :, None], 0.0), axis=1)
    return jnp.transpose(table.reshape(table.shape[0], expert_count // n, n), (2, 0, 1))


def body(
    queries,
    key_nope,
    key_rope,
    values,
    residual,
    segments,
    out_proj,
    norm_gain,
    expert_gate,
    expert_up,
    expert_down,
    routes,
    route_weights,
):
    half_rows, stream_count, _ = queries.shape
    model_width = residual.shape[2]
    token_rows = half_rows * stream_count
    expert_count = lax.axis_size(EXPERT)
    items = stream_count * HEADS

    def by_stream(array):
        array = array.reshape(half_rows, stream_count, array.shape[-1])
        return jnp.swapaxes(array, 0, 1).reshape(token_rows, array.shape[-1])

    query_items = queries.reshape(half_rows, items, NOPE + ROPE)
    rope_items = jnp.broadcast_to(key_rope[:, :, None, :], (half_rows, stream_count, HEADS, ROPE))
    packed = jnp.concatenate(
        [
            query_items[:, :, :NOPE],
            key_nope.reshape(half_rows, items, NOPE),
            values.reshape(half_rows, items, V_DIM),
            query_items[:, :, NOPE:],
            rope_items.reshape(half_rows, items, ROPE),
        ],
        axis=2,
    )
    borders = jnp.sum((segments == 0).astype(jnp.int32), axis=1)
    mine = jnp.arange(stream_count, dtype=jnp.int32) == lax.axis_index(EXPERT) // HEADS
    bound = jnp.sum(jnp.where(mine, borders, 0)).reshape(1)
    own_weights = (expert_gate[0].T, expert_up[0].T, expert_down[0])
    table = column_table(
        by_stream(routes[0, 0]), by_stream(route_weights[0, 0]), expert_count, lax.axis_size("z")
    )
    attn_rows, weight_table, other_weights = attend_and_gather(
        jnp.swapaxes(packed, 0, 1), bound, table, own_weights
    )
    projected = jnp.dot(
        attn_rows,
        lax.all_gather(out_proj, DP + EXPERT, axis=0, tiled=True),
        preferred_element_type=jnp.float32,
    )
    hidden = by_stream(residual).astype(jnp.float32) + projected
    mean_square = jnp.mean(hidden * hidden, axis=1, keepdims=True)
    normed = (hidden * lax.rsqrt(mean_square + EPSILON) * norm_gain.astype(jnp.float32)).astype(
        jnp.bfloat16
    )
    layer_out = mix_experts(normed, hidden, weight_table, own_weights, other_weights)
    return jnp.swapaxes(layer_out.reshape(stream_count, half_rows, model_width), 0, 1)


def solution(mesh):
    split = Mesh(mesh.devices.reshape(4, 2, 4, 8), DP + EXPERT)
    rows = P(EXPERT, DP, None)
    weights = P(EXPERT, None, None)
    pairs = P(DP, EXPERT, None, None)
    return jax.shard_map(
        body,
        mesh=split,
        in_specs=(
            rows,
            rows,
            rows,
            rows,
            rows,
            P(DP, None),
            P(DP + EXPERT, None),
            P(),
            weights,
            weights,
            weights,
            pairs,
            pairs,
        ),
        out_specs=rows,
        check_vma=False,
    )
```

```python
import functools

import jax
import jax.numpy as jnp
from jax import lax
from jax.experimental import pallas as pl
from jax.experimental.pallas import tpu as pltpu
from jax.sharding import Mesh, PartitionSpec as P

MESH = pl.DeviceIdType.MESH
DP = ("x", "core")
EXPERT = ("y", "z")

HEADS = 16
NOPE = 128
ROPE = 64
V_DIM = 128
TOP = 6


EPSILON = 1e-06
QUERY_BLOCK = 512


def front_kernel(queries, keys, values, ropes, bound, table, proj, own_g, own_u, own_d,
                 attn_ref, tab_ref, others, proj_all,
                 rows_buf, qbuf, kbuf, att, local_sem, a2a_sem, att_sem, tab_sem,
                 ysend, yrecv, xsend, xrecv, csend, crecv, psend, precv):
    size_x, size_y, size_z = lax.axis_size("x"), lax.axis_size("y"), lax.axis_size("z")
    peers = size_y * size_z
    x, core = lax.axis_index("x"), lax.axis_index("core")
    y, z = lax.axis_index("y"), lax.axis_index("z")
    me = y * size_z + z
    up_y, down_y = {"y": lax.rem(y + 1, size_y)}, {"y": lax.rem(y + size_y - 1, size_y)}
    up_x, down_x = {"x": lax.rem(x + 1, size_x)}, {"x": lax.rem(x + size_x - 1, size_x)}
    other_core = {"core": 1 - core}
    packed = (queries, keys, values, ropes)
    block = queries.shape[1]
    heads = attn_ref.shape[1] // V_DIM
    ff, width = own_d.shape
    high, wide = ff // size_x, width // 4

    def peer(e):
        return {"y": lax.div(e, size_z), "z": lax.rem(e, size_z)}

    def remote(src, dst, send, recv, device):
        return pltpu.make_async_remote_copy(
            src_ref=src, dst_ref=dst, send_sem=send, recv_sem=recv, device_id=device, device_id_type=MESH
        )

    barrier = pltpu.get_barrier_semaphore()

    def greet(d, carry):
        pl.semaphore_signal(barrier, inc=1, device_id=peer(lax.rem(me + d, peers)), device_id_type=MESH)
        return carry

    lax.fori_loop(1, peers, greet, 0)
    for device in (up_x, down_x, other_core):
        pl.semaphore_signal(barrier, inc=1, device_id=device, device_id_type=MESH)
    pl.semaphore_wait(barrier, peers + 2)

    def blocks(first, amount):
        return proj_all.at[pl.ds(first, amount)]

    own_block = ((x * 2 + core) * size_y + y) * size_z + z
    group = peers

    def group_of(gx, gcore):
        return (lax.rem(gx + size_x, size_x) * 2 + gcore) * group

    def proj_copy(n, first, amount, device):
        return remote(blocks(first, amount), blocks(first, amount), psend.at[n], precv.at[n], device)

    for d in range(1, size_z):
        remote(proj, proj_all.at[own_block], psend.at[0], precv.at[0], {"z": lax.rem(z + d, size_z)}).start()
    own_proj = pltpu.make_async_copy(proj, proj_all.at[own_block], local_sem.at[3])
    own_proj.start()

    def rows_of(e):
        return pl.ds(pl.multiple_of(e * block, block), block)

    def send_rows(d, carry):
        e = lax.rem(me + d, peers)
        for i, part in enumerate(packed):
            place = rows_buf.at[rows_of(me), pl.ds(i * 128, 128)]
            remote(part.at[e], place, a2a_sem.at[0], a2a_sem.at[1], peer(e)).start()
        return carry

    lax.fori_loop(1, peers, send_rows, 0)
    for i, part in enumerate(packed):
        place = rows_buf.at[rows_of(me), pl.ds(i * 128, 128)]
        pltpu.make_async_copy(part.at[me], place, local_sem.at[0]).start()

    own_proj.wait()
    proj_copy(0, 0, size_z - 1, up_y).wait_recv()
    for d in range(1, size_y):
        proj_copy(1, own_block - z, size_z, {"y": lax.rem(y + d, size_y)}).start()

    def columns(u):
        return pl.ds(pl.multiple_of((core * 2 + u) * wide, wide), wide)

    def region(s, q, u):
        return others.at[s, :, pl.ds(q * high, high), columns(u)]

    def y_index(s, q, u):
        return (s * 2 + q) * 2 + u

    def y_start(s, q, u):
        n = y_index(s, q, u)
        quarter = pl.ds(pl.multiple_of(lax.rem(x + q, size_x) * high, high), high)
        for m, own in enumerate((own_g, own_u, own_d)):
            remote(
                own.at[quarter, columns(u)],
                others.at[s, m, pl.ds(q * high, high), columns(u)],
                ysend.at[n],
                yrecv.at[n],
                up_y if s == 0 else down_y,
            ).start()

    def y_copy(s, q, u):
        n = y_index(s, q, u)
        return remote(region(s, q, u), region(s, q, u), ysend.at[n], yrecv.at[n], up_y)

    def x_copy(s, q, u):
        device, slot = (up_x, 3) if q == 0 else (down_x, 2)
        n = (s * 2 + q) * 2 + u
        return remote(region(s, q, u), region(s, slot, u), xsend.at[n], xrecv.at[n], device)

    def c_copy(s, q, u):
        n = (s * 4 + q) * 2 + u
        return remote(region(s, q, u), region(s, q, u), csend.at[n], crecv.at[n], other_core)

    for first in (True, False):
        for u in range(2):
            for s in range(2):
                y_start(s, s if first else 1 - s, u)

    def tab_copy(d):
        to = lax.rem(z + d, size_z)
        return remote(table.at[to], tab_ref.at[z], tab_sem.at[0], tab_sem.at[1], {"z": to})

    for d in range(1, size_z):
        tab_copy(d).start()
    own_table = pltpu.make_async_copy(table.at[z], tab_ref.at[z], local_sem.at[1])
    own_table.start()

    proj_copy(1, 0, (size_y - 1) * size_z, up_y).wait_recv()
    for n, device in ((2, up_x), (3, down_x), (4, other_core)):
        proj_copy(n, group_of(x, core), group, device).start()

    def arrived(s, q, u):
        x_copy(s, q, u).start()
        c_copy(s, q, u).start()

    for u in range(2):
        for s in range(2):
            y_copy(s, s, u).wait_recv()
            arrived(s, s, u)

    half_group = group // 2
    proj_copy(2, group_of(x - 1, core), group, up_x).wait_recv()
    proj_copy(5, group_of(x - 1, core), half_group, up_x).start()
    proj_copy(7, group_of(x - 1, core), group, other_core).start()
    proj_copy(3, group_of(x + 1, core), group, up_x).wait_recv()
    proj_copy(6, group_of(x + 1, core) + half_group, half_group, down_x).start()
    proj_copy(8, group_of(x + 1, core), group, other_core).start()

    own_place = rows_buf.at[rows_of(me)]
    pltpu.make_async_copy(own_place, own_place, local_sem.at[0]).wait()
    most = rows_buf.at[pl.ds(0, (peers - 1) * block)]
    remote(most, most, a2a_sem.at[0], a2a_sem.at[1], up_y).wait_recv()

    length = rows_buf.shape[0]
    lane = lax.broadcasted_iota(jnp.int32, (1, 128), 1)
    swap = (
        lax.broadcasted_iota(jnp.int32, (128, 128), 0) == lax.broadcasted_iota(jnp.int32, (128, 128), 1) + ROPE
    ).astype(jnp.bfloat16)

    step = min(512, length)
    strip = min(256, step)

    def arrange(i, carry):
        span = pl.ds(pl.multiple_of(i * step, step), step)
        rope = rows_buf[span, 384:512]
        qbuf[span, 0:128] = rows_buf[span, 0:128]
        qbuf[span, 128:256] = jnp.where(lane < ROPE, rope, jnp.zeros_like(rope))
        kbuf[span, 0:128] = rows_buf[span, 128:256]
        kbuf[span, 128:256] = jnp.dot(rope, swap, preferred_element_type=jnp.float32).astype(jnp.bfloat16)
        return carry

    lax.fori_loop(0, length // step, arrange, 0)
    border = bound[0]
    scale = (NOPE + ROPE) ** (-0.5)
    stream, head = lax.div(me, heads), lax.rem(me, heads)
    target = (
        pl.ds(pl.multiple_of(stream * block, block), block),
        pl.ds(pl.multiple_of(head * V_DIM, V_DIM), V_DIM),
    )

    def back_copy(e):
        return remote(att.at[rows_of(e)], attn_ref.at[target[0], target[1]], att_sem.at[0], att_sem.at[1], peer(e))

    def local_back():
        return pltpu.make_async_copy(att.at[rows_of(me)], attn_ref.at[target[0], target[1]], local_sem.at[2])

    def attend(i):
        limit = (i + 1) * step

        def one(j, carry):
            first = i * step + j * strip
            span = pl.ds(pl.multiple_of(first, strip), strip)
            scores = lax.dot_general(
                qbuf[span, :], kbuf[0:limit, :], (((1,), (1,)), ((), ())), preferred_element_type=jnp.float32
            ) * scale
            row = first + lax.broadcasted_iota(jnp.int32, (strip, 1), 0)
            column = lax.broadcasted_iota(jnp.int32, (1, limit), 1)
            lowest = jnp.where(row >= border, border, 0)
            scores = jnp.where((column <= row) & (column >= lowest), scores, -jnp.inf)
            raised = jnp.exp(scores - jnp.max(scores, axis=1, keepdims=True))
            total = jnp.sum(raised, axis=1, keepdims=True)
            mixed = jnp.dot(
                raised.astype(jnp.bfloat16), rows_buf[0:limit, 256:384], preferred_element_type=jnp.float32
            )
            att[span, :] = (mixed / total).astype(jnp.bfloat16)
            for t in range(strip // block):
                e = lax.div(first, block) + t

                @pl.when(e != me)
                def _():
                    back_copy(e).start()

                @pl.when(e == me)
                def _():
                    local_back().start()

            return carry

        lax.fori_loop(0, step // strip, one, 0)

    count = length // step
    for i in range(count):
        attend(i)
        if i == count // 2 - 1:
            for u in range(2):
                for s in range(2):
                    y_copy(s, 1 - s, u).wait_recv()
                    arrived(s, 1 - s, u)

    def crossed(s, q, u):
        x_copy(s, q, u).wait_recv()
        c_copy(s, 3 if q == 0 else 2, u).start()

    proj_copy(5, 0, half_group, up_x).wait_recv()
    proj_copy(9, group_of(x + 2, core), half_group, other_core).start()
    proj_copy(6, 0, half_group, up_x).wait_recv()
    proj_copy(10, group_of(x + 2, core) + half_group, half_group, other_core).start()
    for u in range(2):
        for s in range(2):
            crossed(s, s, u)
    for u in range(2):
        for s in range(2):
            crossed(s, 1 - s, u)

    for s in range(2):
        for q in range(4):
            for u in range(2):
                c_copy(s, q, u).wait()
    for u in range(2):
        for q in range(2):
            for s in range(2):
                y_copy(s, q, u).wait_send()
                x_copy(s, q, u).wait_send()
    proj_copy(0, 0, size_z - 1, up_y).wait_send()
    proj_copy(1, 0, (size_y - 1) * size_z, up_y).wait_send()
    for n, amount in ((2, group), (3, group), (5, half_group), (6, half_group)):
        proj_copy(n, 0, amount, up_x).wait_send()
    for n, amount in ((4, group), (7, group), (8, group), (9, half_group), (10, half_group)):
        proj_copy(n, 0, amount, other_core).wait()
    remote(most, most, a2a_sem.at[0], a2a_sem.at[1], up_y).wait_send()
    local_back().wait()
    back = att.at[pl.ds(0, (peers - 1) * block)]
    remote(back, back, att_sem.at[0], att_sem.at[1], up_y).wait()
    own_table.wait()
    tables = tab_ref.at[pl.ds(0, size_z - 1)]
    remote(tables, tables, tab_sem.at[0], tab_sem.at[1], up_y).wait()


def attend_and_gather(packed, bound, table, proj, own_weights):
    peers, block, _ = packed[0].shape
    ff, width = own_weights[2].shape
    heads = width // V_DIM
    length = peers * block
    vmem = pl.BlockSpec(memory_space=pltpu.VMEM)
    anywhere = pl.BlockSpec(memory_space=pl.ANY)
    dma = pltpu.SemaphoreType.DMA
    return pl.pallas_call(
        front_kernel,
        out_shape=(
            jax.ShapeDtypeStruct((peers // heads * block, width), jnp.bfloat16),
            jax.ShapeDtypeStruct(table.shape, jnp.float32),
            jax.ShapeDtypeStruct((2, 3, ff, width), jnp.bfloat16),
            jax.ShapeDtypeStruct((width // proj.shape[0],) + proj.shape, jnp.bfloat16),
        ),
        in_specs=[anywhere] * 4 + [pl.BlockSpec(memory_space=pltpu.SMEM), vmem] + [anywhere] * 4,
        out_specs=(vmem, vmem, anywhere, anywhere),
        scratch_shapes=[
            pltpu.VMEM((length, 512), jnp.bfloat16),
            pltpu.VMEM((length, 256), jnp.bfloat16),
            pltpu.VMEM((length, 256), jnp.bfloat16),
            pltpu.VMEM((length, V_DIM), jnp.bfloat16),
            dma((4,)),
            dma((2,)),
            dma((2,)),
            dma((2,)),
            dma((8,)),
            dma((8,)),
            dma((8,)),
            dma((8,)),
            dma((16,)),
            dma((16,)),
            dma((11,)),
            dma((11,)),
        ],
        compiler_params=pltpu.CompilerParams(
            collective_id=1, has_side_effects=True, vmem_limit_bytes=50000000
        ),
        cost_estimate=pl.CostEstimate(flops=100000000000, bytes_accessed=40000000, transcendentals=0),
    )(*packed, bound, table, proj, *own_weights)


def moe_kernel(axis_size, x_ref, hid_ref, wt_ref, own_g, own_u, own_d, others,
               out_ref, xbuf, acc, act, weights, rbuf, lbuf, start_sem, send_sem, recv_sem, wsem,
               fsend, frecv, xsend, xrecv, csend, crecv):
    n = axis_size
    half_n = n // 2
    y, z = lax.axis_index("y"), lax.axis_index("z")
    right = {"z": lax.rem(z + 1, n)}
    left = {"z": lax.rem(z + n - 1, n)}
    rows = x_ref.shape[0]
    half = rows // 2
    count, _, ff, width = weights.shape
    sent = 2 * half_n - 1

    def slot(d):
        return lax.rem(z + 2 * n - d, n)

    def part(c):
        return pl.ds(pl.multiple_of(c * half, half), half)

    for i, own in enumerate((own_g, own_u, own_d)):
        pltpu.make_async_copy(own, weights.at[0, i], wsem.at[0]).start()
    last = count - 1
    for k in range(1, last):
        pltpu.make_async_copy(others.at[k - 1], weights.at[k], wsem.at[k]).start()

    size_x, size_y = lax.axis_size("x"), lax.axis_size("y")
    x, core = lax.axis_index("x"), lax.axis_index("core")
    up_y, down_y = {"y": lax.rem(y + 1, size_y)}, {"y": lax.rem(y + size_y - 1, size_y)}
    up_x, down_x = {"x": lax.rem(x + 1, size_x)}, {"x": lax.rem(x + size_x - 1, size_x)}
    other_core = {"core": 1 - core}
    barrier = pltpu.get_barrier_semaphore()
    for neighbour in (left, right, up_y, down_y, up_x, down_x, other_core):
        pl.semaphore_signal(barrier, inc=1, device_id=neighbour, device_id_type=MESH)
    pl.semaphore_wait(barrier, 7)

    def gather_copy(j, way):
        d = j // 2
        c = lax.rem(j + way, 2)
        source = slot(d) if way == 0 else slot(n - d)
        return pltpu.make_async_remote_copy(
            src_ref=xbuf.at[source, part(c)],
            dst_ref=xbuf.at[source, part(c)],
            send_sem=send_sem.at[way, j],
            recv_sem=recv_sem.at[way, j],
            device_id=right if way == 0 else left,
            device_id_type=MESH,
        )

    def gather_arrival(j, way):
        d = j // 2 + 1
        c = lax.rem(j + way, 2)
        source = slot(d) if way == 0 else slot(n - d)
        return pltpu.make_async_remote_copy(
            src_ref=xbuf.at[source, part(c)],
            dst_ref=xbuf.at[source, part(c)],
            send_sem=send_sem.at[way, j],
            recv_sem=recv_sem.at[way, j],
            device_id=right if way == 0 else left,
            device_id_type=MESH,
        )

    own_copy = pltpu.make_async_copy(x_ref, xbuf.at[z], start_sem)
    own_copy.start()
    own_copy.wait()
    for j in range(2):
        for way in range(2):
            gather_copy(j, way).start()

    high, wide = ff // size_x, width // 4

    def section(ref, k, q, u):
        columns = pl.ds(pl.multiple_of((core * 2 + u) * wide, wide), wide)
        return ref.at[k, :, pl.ds(q * high, high), columns]

    def remote(src, dst, send, recv, device):
        return pltpu.make_async_remote_copy(
            src_ref=src, dst_ref=dst, send_sem=send, recv_sem=recv, device_id=device, device_id_type=MESH
        )

    def f_copy(q, u):
        n = q * 2 + u
        return remote(
            section(others, q, q, u), section(weights, last, q, u), fsend.at[n], frecv.at[n],
            up_y if q == 0 else down_y,
        )

    def x_copy(q, u):
        n = q * 2 + u
        device, slot = (up_x, 3) if q == 0 else (down_x, 2)
        return remote(section(weights, last, q, u), section(weights, last, slot, u), xsend.at[n], xrecv.at[n], device)

    def c_copy(q, u):
        n = q * 2 + u
        return remote(section(weights, last, q, u), section(weights, last, q, u), csend.at[n], crecv.at[n], other_core)

    def arrived(u):
        for q in range(2):
            f_copy(q, u).wait_recv()
            x_copy(q, u).start()
            c_copy(q, u).start()

    def crossed(u):
        for q in range(2):
            x_copy(q, u).wait_recv()
            c_copy(3 if q == 0 else 2, u).start()

    for u in range(2):
        for q in range(2):
            f_copy(q, u).start()

    def pass_on(j):
        for way in range(2):
            gather_arrival(j, way).wait_recv()

        @pl.when(j + 2 < sent)
        def _():
            for way in range(2):
                gather_copy(j + 2, way).start()

    lanes = lax.broadcasted_iota(jnp.int32, (1, wt_ref.shape[2]), 1)
    cuts = [(a, min(a + 256, ff)) for a in range(0, ff, 256)]

    def gate_up(slots, k):
        x = jnp.concatenate([xbuf[s] for s in slots], axis=0) if len(slots) > 1 else xbuf[slots[0]]
        wrow = jnp.concatenate([wt_ref[s] for s in slots], axis=0) if len(slots) > 1 else wt_ref[slots[0]]
        offset = jnp.where(k == 0, 0, jnp.where(k == 1, count - 1, k - 1))
        scale = jnp.sum(jnp.where(lanes == lax.rem(y + offset, count), wrow, 0.0), axis=1, keepdims=True)
        m = x.shape[0]

        def product(which, lo, hi):
            return lax.dot_general(
                x, weights[k, which, lo:hi], (((1,), (1,)), ((), ())), preferred_element_type=jnp.float32
            )

        for lo, hi in cuts:
            g, u = product(0, lo, hi), product(1, lo, hi)
            a = g / (1.0 + jnp.exp(-g)) * u * scale
            act[k, 0:m, lo:hi] = a.astype(jnp.bfloat16)

    def down(slots, experts, more):
        m = rows * len(slots)

        def columns(q, carry):
            span = pl.ds(pl.multiple_of(q * 512, min(512, width)), min(512, width))
            y = jnp.dot(act[experts[0], 0:m, :], weights[experts[0], 2, :, span], preferred_element_type=jnp.float32)
            for k in experts[1:]:
                y += jnp.dot(act[k, 0:m, :], weights[k, 2, :, span], preferred_element_type=jnp.float32)
            for i, s in enumerate(slots):
                part_y = y[i * rows:(i + 1) * rows]
                if more:
                    part_y += acc[s, :, span].astype(jnp.float32)
                acc[s, :, span] = part_y.astype(jnp.bfloat16)
            return carry

        lax.fori_loop(0, max(1, width // 512), columns, 0)

    def fetched(k):
        whole = weights.at[k]
        pltpu.make_async_copy(whole, whole, wsem.at[k]).wait()

    def own_step(k, carry):
        fetched(k)
        gate_up([z], k)

        @pl.when(k == 1)
        def _():
            pass_on(0)

        return carry

    early = tuple(range(last))
    lax.fori_loop(0, last, own_step, 0)
    down([z], early, False)
    arrived(0)

    def pair_step(p, carry):
        pass_on(2 * p - 1)
        slots = [slot(p), slot(n - p)]

        def one(k, inner):
            gate_up(slots, k)

            @pl.when(k == 1)
            def _():
                pass_on(2 * p)

            return inner

        lax.fori_loop(0, last, one, 0)
        down(slots, early, False)

        @pl.when(p == 1)
        def _():
            arrived(1)

        @pl.when(p == 2)
        def _():
            crossed(0)

        @pl.when(p == 3)
        def _():
            crossed(1)

        return carry

    lax.fori_loop(1, half_n, pair_step, 0)
    far = [slot(half_n)]

    def far_step(k, carry):
        gate_up(far, k)
        return carry

    lax.fori_loop(0, last, far_step, 0)
    down(far, early, False)
    for q in range(4):
        for u in range(2):
            c_copy(q, u).wait_recv()

    def finish(slots):
        gate_up(slots, last)
        down(slots, (last,), True)

    finish(far)
    bufs = (rbuf, lbuf)

    def sum_copy(j, way):
        return pltpu.make_async_remote_copy(
            src_ref=bufs[way].at[sent + j if j < 2 else j - 2],
            dst_ref=bufs[way].at[j],
            send_sem=send_sem.at[way, sent + j],
            recv_sem=recv_sem.at[way, sent + j],
            device_id=right if way == 0 else left,
            device_id_type=MESH,
        )

    def send_sums(j):
        for way in range(2):
            off = half_n - (j + 1) // 2
            owner = slot(n - off) if way == 0 else slot(off)
            c = (j + way) % 2
            own_part = acc[owner, part(c)]
            if j < 2:
                bufs[way][sent + j] = own_part
            else:
                sum_copy(j - 2, way).wait_recv()
                bufs[way][j - 2] = (bufs[way][j - 2].astype(jnp.float32) + own_part.astype(jnp.float32)).astype(jnp.bfloat16)
            sum_copy(j, way).start()

    send_sums(0)
    for p in range(half_n - 1, 0, -1):
        finish([slot(p), slot(n - p)])
        j = 2 * (half_n - p) - 1
        send_sums(j)
        send_sums(j + 1)
    finish([z])
    for way in range(2):
        for j in (sent - 2, sent - 1):
            sum_copy(j, way).wait_recv()
    for c in range(2):
        total = hid_ref[part(c)] + acc[z, part(c)].astype(jnp.float32)
        for way in range(2):
            j = sent - 1 if (sent - 1 + way) % 2 == c else sent - 2
            total += bufs[way][j].astype(jnp.float32)
        out_ref[part(c)] = total.astype(jnp.bfloat16)
    for j in range(sent):
        for way in range(2):
            gather_copy(j, way).wait_send()
            sum_copy(j, way).wait_send()
    for q in range(4):
        for u in range(2):
            c_copy(q, u).wait_send()
            if q < 2:
                f_copy(q, u).wait_send()
                x_copy(q, u).wait_send()


def mix_experts(normed, hidden, weight_table, own_weights, other_weights):
    rows, width = normed.shape
    n = lax.axis_size("z")
    ff = own_weights[2].shape[0]
    count = 2 + other_weights.shape[0]
    sent = n - 1
    vmem = pl.BlockSpec(memory_space=pltpu.VMEM)
    anywhere = pl.BlockSpec(memory_space=pl.ANY)
    return pl.pallas_call(
        functools.partial(moe_kernel, n),
        out_shape=jax.ShapeDtypeStruct((rows, width), jnp.bfloat16),
        in_specs=[vmem] * 3 + [anywhere] * 4,
        out_specs=vmem,
        scratch_shapes=[
            pltpu.VMEM((n, rows, width), jnp.bfloat16),
            pltpu.VMEM((n, rows, width), jnp.bfloat16),
            pltpu.VMEM((count, 2 * rows, ff), jnp.bfloat16),
            pltpu.VMEM((count, 3, ff, width), jnp.bfloat16),
            pltpu.VMEM((sent + 2, rows // 2, width), jnp.bfloat16),
            pltpu.VMEM((sent + 2, rows // 2, width), jnp.bfloat16),
            pltpu.SemaphoreType.DMA,
            pltpu.SemaphoreType.DMA((2, 2 * sent)),
            pltpu.SemaphoreType.DMA((2, 2 * sent)),
            pltpu.SemaphoreType.DMA((count,)),
        ] + [pltpu.SemaphoreType.DMA((4,))] * 4 + [
            pltpu.SemaphoreType.DMA((8,)),
            pltpu.SemaphoreType.DMA((8,)),
        ],
        compiler_params=pltpu.CompilerParams(
            collective_id=0, has_side_effects=True, vmem_limit_bytes=66000000
        ),
        cost_estimate=pl.CostEstimate(
            flops=6 * n * rows * width * ff * count, bytes_accessed=40000000, transcendentals=0
        ),
    )(normed, hidden, weight_table, *own_weights, other_weights)


def column_table(routes, route_weights, expert_count, n):
    experts = jnp.arange(expert_count, dtype=jnp.int32)
    chosen = routes[:, :, None] == experts[None, None, :]
    table = jnp.sum(jnp.where(chosen, route_weights[:, :, None], 0.0), axis=1)
    return jnp.transpose(table.reshape(table.shape[0], expert_count // n, n), (2, 0, 1))


def body(
    queries,
    key_nope,
    key_rope,
    values,
    residual,
    segments,
    out_proj,
    norm_gain,
    expert_gate,
    expert_up,
    expert_down,
    routes,
    route_weights,
):
    half_rows, stream_count, _ = queries.shape
    model_width = residual.shape[2]
    token_rows = half_rows * stream_count
    expert_count = lax.axis_size(EXPERT)
    items = stream_count * HEADS

    def by_stream(array):
        array = array.reshape(half_rows, stream_count, array.shape[-1])
        return jnp.swapaxes(array, 0, 1).reshape(token_rows, array.shape[-1])

    query_items = queries.reshape(half_rows, items, NOPE + ROPE)
    rope_items = jnp.broadcast_to(key_rope[:, :, None, :], (half_rows, stream_count, HEADS, ROPE))
    ropes = jnp.concatenate(
        [query_items[:, :, NOPE:], rope_items.reshape(half_rows, items, ROPE)], axis=2
    )
    packed = [
        jnp.swapaxes(part, 0, 1)
        for part in (
            query_items[:, :, :NOPE],
            key_nope.reshape(half_rows, items, NOPE),
            values.reshape(half_rows, items, V_DIM),
            ropes,
        )
    ]
    borders = jnp.sum((segments == 0).astype(jnp.int32), axis=1)
    mine = jnp.arange(stream_count, dtype=jnp.int32) == lax.axis_index(EXPERT) // HEADS
    bound = jnp.sum(jnp.where(mine, borders, 0)).reshape(1)
    own_weights = (expert_gate[0].T, expert_up[0].T, expert_down[0])
    table = column_table(
        by_stream(routes[0, 0]), by_stream(route_weights[0, 0]), expert_count, lax.axis_size("z")
    )
    attn_rows, weight_table, other_weights, proj_all = attend_and_gather(
        packed, bound, table, out_proj, own_weights
    )
    projected = jnp.dot(
        attn_rows, proj_all.reshape(model_width, model_width), preferred_element_type=jnp.float32
    )
    hidden = by_stream(residual).astype(jnp.float32) + projected
    mean_square = jnp.mean(hidden * hidden, axis=1, keepdims=True)
    normed = (hidden * lax.rsqrt(mean_square + EPSILON) * norm_gain.astype(jnp.float32)).astype(
        jnp.bfloat16
    )
    layer_out = mix_experts(normed, hidden, weight_table, own_weights, other_weights)
    return jnp.swapaxes(layer_out.reshape(stream_count, half_rows, model_width), 0, 1)


def solution(mesh):
    split = Mesh(mesh.devices.reshape(4, 2, 4, 8), DP + EXPERT)
    rows = P(EXPERT, DP, None)
    weights = P(EXPERT, None, None)
    pairs = P(DP, EXPERT, None, None)
    return jax.shard_map(
        body,
        mesh=split,
        in_specs=(
            rows,
            rows,
            rows,
            rows,
            rows,
            P(DP, None),
            P(DP + EXPERT, None),
            P(),
            weights,
            weights,
            weights,
            pairs,
            pairs,
        ),
        out_specs=rows,
        check_vma=False,
    )
```

```python
import functools

import jax
import jax.numpy as jnp
from jax import lax
from jax.experimental import pallas as pl
from jax.experimental.pallas import tpu as pltpu
from jax.sharding import Mesh, PartitionSpec as P

MESH = pl.DeviceIdType.MESH
DP = ("x", "core")
EXPERT = ("y", "z")

HEADS = 16
NOPE = 128
ROPE = 64
V_DIM = 128
TOP = 6


EPSILON = 1e-06
QUERY_BLOCK = 512


def front_kernel(queries, keys, values, ropes, bound, table, proj, own_g, own_u, own_d,
                 attn_ref, tab_ref, others, proj_all,
                 rows_buf, qbuf, kbuf, att, local_sem, a2a_sem, att_sem, tab_sem,
                 ysend, yrecv, xsend, xrecv, csend, crecv, psend, precv):
    size_x, size_y, size_z = lax.axis_size("x"), lax.axis_size("y"), lax.axis_size("z")
    peers = size_y * size_z
    x, core = lax.axis_index("x"), lax.axis_index("core")
    y, z = lax.axis_index("y"), lax.axis_index("z")
    me = y * size_z + z
    up_y, down_y = {"y": lax.rem(y + 1, size_y)}, {"y": lax.rem(y + size_y - 1, size_y)}
    up_x, down_x = {"x": lax.rem(x + 1, size_x)}, {"x": lax.rem(x + size_x - 1, size_x)}
    other_core = {"core": 1 - core}
    packed = (queries, keys, values, ropes)
    block = queries.shape[1]
    heads = attn_ref.shape[1] // V_DIM
    ff, width = own_d.shape
    high, wide = ff // size_x, width // 4

    def peer(e):
        return {"y": lax.div(e, size_z), "z": lax.rem(e, size_z)}

    def remote(src, dst, send, recv, device):
        return pltpu.make_async_remote_copy(
            src_ref=src, dst_ref=dst, send_sem=send, recv_sem=recv, device_id=device, device_id_type=MESH
        )

    barrier = pltpu.get_barrier_semaphore()

    def greet(d, carry):
        pl.semaphore_signal(barrier, inc=1, device_id=peer(lax.rem(me + d, peers)), device_id_type=MESH)
        return carry

    lax.fori_loop(1, peers, greet, 0)
    for device in (up_x, down_x, other_core):
        pl.semaphore_signal(barrier, inc=1, device_id=device, device_id_type=MESH)
    pl.semaphore_wait(barrier, peers + 2)

    def blocks(first, amount):
        return proj_all.at[pl.ds(first, amount)]

    own_block = ((x * 2 + core) * size_y + y) * size_z + z
    group = peers

    def group_of(gx, gcore):
        return (lax.rem(gx + size_x, size_x) * 2 + gcore) * group

    def proj_copy(n, first, amount, device):
        return remote(blocks(first, amount), blocks(first, amount), psend.at[n], precv.at[n], device)

    for d in range(1, size_z):
        remote(proj, proj_all.at[own_block], psend.at[0], precv.at[0], {"z": lax.rem(z + d, size_z)}).start()
    own_proj = pltpu.make_async_copy(proj, proj_all.at[own_block], local_sem.at[3])
    own_proj.start()

    def rows_of(e):
        return pl.ds(pl.multiple_of(e * block, block), block)

    def send_rows(d, carry):
        e = lax.rem(me + d, peers)
        for i, part in enumerate(packed):
            place = rows_buf.at[rows_of(me), pl.ds(i * 128, 128)]
            remote(part.at[e], place, a2a_sem.at[0], a2a_sem.at[1], peer(e)).start()
        return carry

    lax.fori_loop(1, peers, send_rows, 0)
    for i, part in enumerate(packed):
        place = rows_buf.at[rows_of(me), pl.ds(i * 128, 128)]
        pltpu.make_async_copy(part.at[me], place, local_sem.at[0]).start()

    own_proj.wait()
    proj_copy(0, 0, size_z - 1, up_y).wait_recv()
    for d in range(1, size_y):
        proj_copy(1, own_block - z, size_z, {"y": lax.rem(y + d, size_y)}).start()

    def columns(u):
        return pl.ds(pl.multiple_of((core * 2 + u) * wide, wide), wide)

    def region(s, q, u):
        return others.at[s, :, pl.ds(q * high, high), columns(u)]

    def y_index(s, q, u):
        return (s * 2 + q) * 2 + u

    def y_start(s, q, u):
        n = y_index(s, q, u)
        quarter = pl.ds(pl.multiple_of(lax.rem(x + q, size_x) * high, high), high)
        for m, own in enumerate((own_g, own_u, own_d)):
            remote(
                own.at[quarter, columns(u)],
                others.at[s, m, pl.ds(q * high, high), columns(u)],
                ysend.at[n],
                yrecv.at[n],
                up_y if s == 0 else down_y,
            ).start()

    def y_copy(s, q, u):
        n = y_index(s, q, u)
        return remote(region(s, q, u), region(s, q, u), ysend.at[n], yrecv.at[n], up_y)

    def x_copy(s, q, u):
        device, slot = (up_x, 3) if q == 0 else (down_x, 2)
        n = (s * 2 + q) * 2 + u
        return remote(region(s, q, u), region(s, slot, u), xsend.at[n], xrecv.at[n], device)

    def c_copy(s, q, u):
        n = (s * 4 + q) * 2 + u
        return remote(region(s, q, u), region(s, q, u), csend.at[n], crecv.at[n], other_core)

    for first in (True, False):
        for u in range(2):
            for s in range(2):
                y_start(s, s if first else 1 - s, u)

    def tab_copy(d):
        to = lax.rem(z + d, size_z)
        return remote(table.at[to], tab_ref.at[z], tab_sem.at[0], tab_sem.at[1], {"z": to})

    for d in range(1, size_z):
        tab_copy(d).start()
    own_table = pltpu.make_async_copy(table.at[z], tab_ref.at[z], local_sem.at[1])
    own_table.start()

    proj_copy(1, 0, (size_y - 1) * size_z, up_y).wait_recv()
    for n, device in ((2, up_x), (3, down_x), (4, other_core)):
        proj_copy(n, group_of(x, core), group, device).start()

    def arrived(s, q, u):
        if s == 0:
            x_copy(s, q, u).start()
            c_copy(s, q, u).start()

    for u in range(2):
        for s in range(2):
            y_copy(s, s, u).wait_recv()
            arrived(s, s, u)

    half_group = group // 2
    proj_copy(2, group_of(x - 1, core), group, up_x).wait_recv()
    proj_copy(5, group_of(x - 1, core), half_group, up_x).start()
    proj_copy(7, group_of(x - 1, core), group, other_core).start()
    proj_copy(3, group_of(x + 1, core), group, up_x).wait_recv()
    proj_copy(6, group_of(x + 1, core) + half_group, half_group, down_x).start()
    proj_copy(8, group_of(x + 1, core), group, other_core).start()

    own_place = rows_buf.at[rows_of(me)]
    pltpu.make_async_copy(own_place, own_place, local_sem.at[0]).wait()
    most = rows_buf.at[pl.ds(0, (peers - 1) * block)]
    remote(most, most, a2a_sem.at[0], a2a_sem.at[1], up_y).wait_recv()

    length = rows_buf.shape[0]
    lane = lax.broadcasted_iota(jnp.int32, (1, 128), 1)
    swap = (
        lax.broadcasted_iota(jnp.int32, (128, 128), 0) == lax.broadcasted_iota(jnp.int32, (128, 128), 1) + ROPE
    ).astype(jnp.bfloat16)

    step = min(512, length)
    strip = min(256, step)

    def arrange(i, carry):
        span = pl.ds(pl.multiple_of(i * step, step), step)
        rope = rows_buf[span, 384:512]
        qbuf[span, 0:128] = rows_buf[span, 0:128]
        qbuf[span, 128:256] = jnp.where(lane < ROPE, rope, jnp.zeros_like(rope))
        kbuf[span, 0:128] = rows_buf[span, 128:256]
        kbuf[span, 128:256] = jnp.dot(rope, swap, preferred_element_type=jnp.float32).astype(jnp.bfloat16)
        return carry

    lax.fori_loop(0, length // step, arrange, 0)
    border = bound[0]
    scale = (NOPE + ROPE) ** (-0.5)
    stream, head = lax.div(me, heads), lax.rem(me, heads)
    target = (
        pl.ds(pl.multiple_of(stream * block, block), block),
        pl.ds(pl.multiple_of(head * V_DIM, V_DIM), V_DIM),
    )

    def back_copy(e):
        return remote(att.at[rows_of(e)], attn_ref.at[target[0], target[1]], att_sem.at[0], att_sem.at[1], peer(e))

    def local_back():
        return pltpu.make_async_copy(att.at[rows_of(me)], attn_ref.at[target[0], target[1]], local_sem.at[2])

    def attend(i):
        limit = (i + 1) * step

        def one(j, carry):
            first = i * step + j * strip
            span = pl.ds(pl.multiple_of(first, strip), strip)
            scores = lax.dot_general(
                qbuf[span, :], kbuf[0:limit, :], (((1,), (1,)), ((), ())), preferred_element_type=jnp.float32
            ) * scale
            row = first + lax.broadcasted_iota(jnp.int32, (strip, 1), 0)
            column = lax.broadcasted_iota(jnp.int32, (1, limit), 1)
            lowest = jnp.where(row >= border, border, 0)
            scores = jnp.where((column <= row) & (column >= lowest), scores, -jnp.inf)
            raised = jnp.exp(scores - jnp.max(scores, axis=1, keepdims=True))
            total = jnp.sum(raised, axis=1, keepdims=True)
            mixed = jnp.dot(
                raised.astype(jnp.bfloat16), rows_buf[0:limit, 256:384], preferred_element_type=jnp.float32
            )
            att[span, :] = (mixed / total).astype(jnp.bfloat16)
            for t in range(strip // block):
                e = lax.div(first, block) + t

                @pl.when(e != me)
                def _():
                    back_copy(e).start()

                @pl.when(e == me)
                def _():
                    local_back().start()

            return carry

        lax.fori_loop(0, step // strip, one, 0)

    count = length // step
    for i in range(count):
        attend(i)

    def crossed(s, q, u):
        x_copy(s, q, u).wait_recv()
        c_copy(s, 3 if q == 0 else 2, u).start()

    proj_copy(5, 0, half_group, up_x).wait_recv()
    proj_copy(9, group_of(x + 2, core), half_group, other_core).start()
    proj_copy(6, 0, half_group, up_x).wait_recv()
    proj_copy(10, group_of(x + 2, core) + half_group, half_group, other_core).start()
    for u in range(2):
        for s in range(2):
            y_copy(s, 1 - s, u).wait_recv()
            arrived(s, 1 - s, u)
    for u in range(2):
        crossed(0, 0, u)
    for u in range(2):
        crossed(0, 1, u)

    for q in range(4):
        for u in range(2):
            c_copy(0, q, u).wait()
    for u in range(2):
        for q in range(2):
            for s in range(2):
                y_copy(s, q, u).wait_send()
            x_copy(0, q, u).wait_send()
    proj_copy(0, 0, size_z - 1, up_y).wait_send()
    proj_copy(1, 0, (size_y - 1) * size_z, up_y).wait_send()
    for n, amount in ((2, group), (3, group), (5, half_group), (6, half_group)):
        proj_copy(n, 0, amount, up_x).wait_send()
    for n, amount in ((4, group), (7, group), (8, group), (9, half_group), (10, half_group)):
        proj_copy(n, 0, amount, other_core).wait()
    remote(most, most, a2a_sem.at[0], a2a_sem.at[1], up_y).wait_send()
    local_back().wait()
    back = att.at[pl.ds(0, (peers - 1) * block)]
    remote(back, back, att_sem.at[0], att_sem.at[1], up_y).wait()
    own_table.wait()
    tables = tab_ref.at[pl.ds(0, size_z - 1)]
    remote(tables, tables, tab_sem.at[0], tab_sem.at[1], up_y).wait()


def attend_and_gather(packed, bound, table, proj, own_weights):
    peers, block, _ = packed[0].shape
    ff, width = own_weights[2].shape
    heads = width // V_DIM
    length = peers * block
    vmem = pl.BlockSpec(memory_space=pltpu.VMEM)
    anywhere = pl.BlockSpec(memory_space=pl.ANY)
    dma = pltpu.SemaphoreType.DMA
    return pl.pallas_call(
        front_kernel,
        out_shape=(
            jax.ShapeDtypeStruct((peers // heads * block, width), jnp.bfloat16),
            jax.ShapeDtypeStruct(table.shape, jnp.float32),
            jax.ShapeDtypeStruct((2, 3, ff, width), jnp.bfloat16),
            jax.ShapeDtypeStruct((width // proj.shape[0],) + proj.shape, jnp.bfloat16),
        ),
        in_specs=[anywhere] * 4 + [pl.BlockSpec(memory_space=pltpu.SMEM), vmem] + [anywhere] * 4,
        out_specs=(vmem, vmem, anywhere, anywhere),
        scratch_shapes=[
            pltpu.VMEM((length, 512), jnp.bfloat16),
            pltpu.VMEM((length, 256), jnp.bfloat16),
            pltpu.VMEM((length, 256), jnp.bfloat16),
            pltpu.VMEM((length, V_DIM), jnp.bfloat16),
            dma((4,)),
            dma((2,)),
            dma((2,)),
            dma((2,)),
            dma((8,)),
            dma((8,)),
            dma((4,)),
            dma((4,)),
            dma((8,)),
            dma((8,)),
            dma((11,)),
            dma((11,)),
        ],
        compiler_params=pltpu.CompilerParams(
            collective_id=1, has_side_effects=True, vmem_limit_bytes=50000000
        ),
        cost_estimate=pl.CostEstimate(flops=100000000000, bytes_accessed=40000000, transcendentals=0),
    )(*packed, bound, table, proj, *own_weights)


def moe_kernel(axis_size, x_ref, hid_ref, wt_ref, own_g, own_u, own_d, others,
               out_ref, xbuf, acc, act, weights, rbuf, lbuf, start_sem, send_sem, recv_sem, wsem,
               fsend, frecv, xsend, xrecv, csend, crecv, lsem):
    n = axis_size
    half_n = n // 2
    y, z = lax.axis_index("y"), lax.axis_index("z")
    right = {"z": lax.rem(z + 1, n)}
    left = {"z": lax.rem(z + n - 1, n)}
    rows = x_ref.shape[0]
    half = rows // 2
    count, _, ff, width = weights.shape
    sent = 2 * half_n - 1

    def slot(d):
        return lax.rem(z + 2 * n - d, n)

    def part(c):
        return pl.ds(pl.multiple_of(c * half, half), half)

    for i, own in enumerate((own_g, own_u, own_d)):
        pltpu.make_async_copy(own, weights.at[0, i], wsem.at[0]).start()
    first_late = count - 2
    for k in range(1, first_late):
        pltpu.make_async_copy(others.at[k - 1], weights.at[k], wsem.at[k]).start()

    size_x, size_y = lax.axis_size("x"), lax.axis_size("y")
    x, core = lax.axis_index("x"), lax.axis_index("core")
    up_y, down_y = {"y": lax.rem(y + 1, size_y)}, {"y": lax.rem(y + size_y - 1, size_y)}
    up_x, down_x = {"x": lax.rem(x + 1, size_x)}, {"x": lax.rem(x + size_x - 1, size_x)}
    other_core = {"core": 1 - core}
    barrier = pltpu.get_barrier_semaphore()
    for neighbour in (left, right, up_y, down_y, up_x, down_x, other_core):
        pl.semaphore_signal(barrier, inc=1, device_id=neighbour, device_id_type=MESH)
    pl.semaphore_wait(barrier, 7)

    def gather_copy(j, way):
        d = j // 2
        c = lax.rem(j + way, 2)
        source = slot(d) if way == 0 else slot(n - d)
        return pltpu.make_async_remote_copy(
            src_ref=xbuf.at[source, part(c)],
            dst_ref=xbuf.at[source, part(c)],
            send_sem=send_sem.at[way, j],
            recv_sem=recv_sem.at[way, j],
            device_id=right if way == 0 else left,
            device_id_type=MESH,
        )

    def gather_arrival(j, way):
        d = j // 2 + 1
        c = lax.rem(j + way, 2)
        source = slot(d) if way == 0 else slot(n - d)
        return pltpu.make_async_remote_copy(
            src_ref=xbuf.at[source, part(c)],
            dst_ref=xbuf.at[source, part(c)],
            send_sem=send_sem.at[way, j],
            recv_sem=recv_sem.at[way, j],
            device_id=right if way == 0 else left,
            device_id_type=MESH,
        )

    own_copy = pltpu.make_async_copy(x_ref, xbuf.at[z], start_sem)
    own_copy.start()
    own_copy.wait()
    for j in range(2):
        for way in range(2):
            gather_copy(j, way).start()

    high, wide = ff // size_x, width // 4
    near, far_k = count - 2, count - 1

    def section(ref, k, q, u):
        columns = pl.ds(pl.multiple_of((core * 2 + u) * wide, wide), wide)
        return ref.at[k, :, pl.ds(q * high, high), columns]

    def remote(src, dst, send, recv, device):
        return pltpu.make_async_remote_copy(
            src_ref=src, dst_ref=dst, send_sem=send, recv_sem=recv, device_id=device, device_id_type=MESH
        )

    def origin(k, q, u):
        return section(others, 1, q, u) if k == near and q < 2 else section(weights, k, q, u)

    def f_copy(q, u):
        n = q * 2 + u
        return remote(
            section(others, q, q, u), section(weights, far_k, q, u), fsend.at[n], frecv.at[n],
            up_y if q == 0 else down_y,
        )

    def x_copy(k, q, u):
        n = ((k - near) * 2 + q) * 2 + u
        device, slot = (up_x, 3) if q == 0 else (down_x, 2)
        return remote(origin(k, q, u), section(weights, k, slot, u), xsend.at[n], xrecv.at[n], device)

    def c_copy(k, q, u):
        n = ((k - near) * 4 + q) * 2 + u
        return remote(origin(k, q, u), section(weights, k, q, u), csend.at[n], crecv.at[n], other_core)

    def local_copy(q, u):
        return pltpu.make_async_copy(section(others, 1, q, u), section(weights, near, q, u), lsem.at[q * 2 + u])

    def arrived(u):
        for q in range(2):
            f_copy(q, u).wait_recv()
            x_copy(far_k, q, u).start()
            c_copy(far_k, q, u).start()

    def crossed(k, u):
        for q in range(2):
            x_copy(k, q, u).wait_recv()
            c_copy(k, 3 if q == 0 else 2, u).start()

    for u in range(2):
        for q in range(2):
            f_copy(q, u).start()
            x_copy(near, q, u).start()
            c_copy(near, q, u).start()
            local_copy(q, u).start()

    def pass_on(j):
        for way in range(2):
            gather_arrival(j, way).wait_recv()

        @pl.when(j + 2 < sent)
        def _():
            for way in range(2):
                gather_copy(j + 2, way).start()

    lanes = lax.broadcasted_iota(jnp.int32, (1, wt_ref.shape[2]), 1)
    cuts = [(a, min(a + 256, ff)) for a in range(0, ff, 256)]

    def gate_up(slots, k):
        x = jnp.concatenate([xbuf[s] for s in slots], axis=0) if len(slots) > 1 else xbuf[slots[0]]
        wrow = jnp.concatenate([wt_ref[s] for s in slots], axis=0) if len(slots) > 1 else wt_ref[slots[0]]
        offset = jnp.where(k == 0, 0, jnp.where(k == 1, count - 1, k - 1))
        scale = jnp.sum(jnp.where(lanes == lax.rem(y + offset, count), wrow, 0.0), axis=1, keepdims=True)
        m = x.shape[0]

        def product(which, lo, hi):
            return lax.dot_general(
                x, weights[k, which, lo:hi], (((1,), (1,)), ((), ())), preferred_element_type=jnp.float32
            )

        for lo, hi in cuts:
            g, u = product(0, lo, hi), product(1, lo, hi)
            a = g / (1.0 + jnp.exp(-g)) * u * scale
            act[k, 0:m, lo:hi] = a.astype(jnp.bfloat16)

    def down(slots, experts, more):
        m = rows * len(slots)

        def columns(q, carry):
            span = pl.ds(pl.multiple_of(q * 512, min(512, width)), min(512, width))
            y = jnp.dot(act[experts[0], 0:m, :], weights[experts[0], 2, :, span], preferred_element_type=jnp.float32)
            for k in experts[1:]:
                y += jnp.dot(act[k, 0:m, :], weights[k, 2, :, span], preferred_element_type=jnp.float32)
            for i, s in enumerate(slots):
                part_y = y[i * rows:(i + 1) * rows]
                if more:
                    part_y += acc[s, :, span].astype(jnp.float32)
                acc[s, :, span] = part_y.astype(jnp.bfloat16)
            return carry

        lax.fori_loop(0, max(1, width // 512), columns, 0)

    def fetched(k):
        whole = weights.at[k]
        pltpu.make_async_copy(whole, whole, wsem.at[k]).wait()

    def own_step(k, carry):
        fetched(k)
        gate_up([z], k)

        @pl.when(k == 1)
        def _():
            pass_on(0)

        return carry

    early, late = tuple(range(near)), (near, far_k)
    lax.fori_loop(0, near, own_step, 0)
    down([z], early, False)
    crossed(near, 0)
    arrived(0)

    def pair_step(p, carry):
        pass_on(2 * p - 1)
        slots = [slot(p), slot(n - p)]

        def one(k, inner):
            gate_up(slots, k)

            @pl.when(k == 1)
            def _():
                pass_on(2 * p)

            return inner

        lax.fori_loop(0, near, one, 0)
        down(slots, early, False)

        @pl.when(p == 1)
        def _():
            crossed(near, 1)
            arrived(1)

        @pl.when(p == 2)
        def _():
            crossed(far_k, 0)

        @pl.when(p == 3)
        def _():
            crossed(far_k, 1)

        return carry

    lax.fori_loop(1, half_n, pair_step, 0)
    far = [slot(half_n)]

    def far_step(k, carry):
        gate_up(far, k)
        return carry

    lax.fori_loop(0, near, far_step, 0)
    down(far, early, False)
    for q in range(4):
        for u in range(2):
            c_copy(near, q, u).wait_recv()
            if q < 2:
                local_copy(q, u).wait()

    def finish(slots, ready=True):
        gate_up(slots, near)
        if not ready:
            for q in range(4):
                for u in range(2):
                    c_copy(far_k, q, u).wait_recv()
        gate_up(slots, far_k)
        down(slots, late, True)

    finish(far, False)
    bufs = (rbuf, lbuf)

    def sum_copy(j, way):
        return pltpu.make_async_remote_copy(
            src_ref=bufs[way].at[sent + j if j < 2 else j - 2],
            dst_ref=bufs[way].at[j],
            send_sem=send_sem.at[way, sent + j],
            recv_sem=recv_sem.at[way, sent + j],
            device_id=right if way == 0 else left,
            device_id_type=MESH,
        )

    def send_sums(j):
        for way in range(2):
            off = half_n - (j + 1) // 2
            owner = slot(n - off) if way == 0 else slot(off)
            c = (j + way) % 2
            own_part = acc[owner, part(c)]
            if j < 2:
                bufs[way][sent + j] = own_part
            else:
                sum_copy(j - 2, way).wait_recv()
                bufs[way][j - 2] = (bufs[way][j - 2].astype(jnp.float32) + own_part.astype(jnp.float32)).astype(jnp.bfloat16)
            sum_copy(j, way).start()

    send_sums(0)
    for p in range(half_n - 1, 0, -1):
        finish([slot(p), slot(n - p)])
        j = 2 * (half_n - p) - 1
        send_sums(j)
        send_sums(j + 1)
    finish([z])
    for way in range(2):
        for j in (sent - 2, sent - 1):
            sum_copy(j, way).wait_recv()
    for c in range(2):
        total = hid_ref[part(c)] + acc[z, part(c)].astype(jnp.float32)
        for way in range(2):
            j = sent - 1 if (sent - 1 + way) % 2 == c else sent - 2
            total += bufs[way][j].astype(jnp.float32)
        out_ref[part(c)] = total.astype(jnp.bfloat16)
    for j in range(sent):
        for way in range(2):
            gather_copy(j, way).wait_send()
            sum_copy(j, way).wait_send()
    for u in range(2):
        for k in late:
            for q in range(4):
                c_copy(k, q, u).wait_send()
            for q in range(2):
                x_copy(k, q, u).wait_send()
        for q in range(2):
            f_copy(q, u).wait_send()


def mix_experts(normed, hidden, weight_table, own_weights, other_weights):
    rows, width = normed.shape
    n = lax.axis_size("z")
    ff = own_weights[2].shape[0]
    count = 2 + other_weights.shape[0]
    sent = n - 1
    vmem = pl.BlockSpec(memory_space=pltpu.VMEM)
    anywhere = pl.BlockSpec(memory_space=pl.ANY)
    return pl.pallas_call(
        functools.partial(moe_kernel, n),
        out_shape=jax.ShapeDtypeStruct((rows, width), jnp.bfloat16),
        in_specs=[vmem] * 3 + [anywhere] * 4,
        out_specs=vmem,
        scratch_shapes=[
            pltpu.VMEM((n, rows, width), jnp.bfloat16),
            pltpu.VMEM((n, rows, width), jnp.bfloat16),
            pltpu.VMEM((count, 2 * rows, ff), jnp.bfloat16),
            pltpu.VMEM((count, 3, ff, width), jnp.bfloat16),
            pltpu.VMEM((sent + 2, rows // 2, width), jnp.bfloat16),
            pltpu.VMEM((sent + 2, rows // 2, width), jnp.bfloat16),
            pltpu.SemaphoreType.DMA,
            pltpu.SemaphoreType.DMA((2, 2 * sent)),
            pltpu.SemaphoreType.DMA((2, 2 * sent)),
            pltpu.SemaphoreType.DMA((count,)),
        ] + [pltpu.SemaphoreType.DMA((amount,)) for amount in (4, 4, 8, 8, 16, 16, 4)] + [
        ],
        compiler_params=pltpu.CompilerParams(
            collective_id=0, has_side_effects=True, vmem_limit_bytes=66000000
        ),
        cost_estimate=pl.CostEstimate(
            flops=6 * n * rows * width * ff * count, bytes_accessed=40000000, transcendentals=0
        ),
    )(normed, hidden, weight_table, *own_weights, other_weights)


def column_table(routes, route_weights, expert_count, n):
    experts = jnp.arange(expert_count, dtype=jnp.int32)
    chosen = routes[:, :, None] == experts[None, None, :]
    table = jnp.sum(jnp.where(chosen, route_weights[:, :, None], 0.0), axis=1)
    return jnp.transpose(table.reshape(table.shape[0], expert_count // n, n), (2, 0, 1))


def body(
    queries,
    key_nope,
    key_rope,
    values,
    residual,
    segments,
    out_proj,
    norm_gain,
    expert_gate,
    expert_up,
    expert_down,
    routes,
    route_weights,
):
    half_rows, stream_count, _ = queries.shape
    model_width = residual.shape[2]
    token_rows = half_rows * stream_count
    expert_count = lax.axis_size(EXPERT)
    items = stream_count * HEADS

    def by_stream(array):
        array = array.reshape(half_rows, stream_count, array.shape[-1])
        return jnp.swapaxes(array, 0, 1).reshape(token_rows, array.shape[-1])

    query_items = queries.reshape(half_rows, items, NOPE + ROPE)
    rope_items = jnp.broadcast_to(key_rope[:, :, None, :], (half_rows, stream_count, HEADS, ROPE))
    ropes = jnp.concatenate(
        [query_items[:, :, NOPE:], rope_items.reshape(half_rows, items, ROPE)], axis=2
    )
    packed = [
        jnp.swapaxes(part, 0, 1)
        for part in (
            query_items[:, :, :NOPE],
            key_nope.reshape(half_rows, items, NOPE),
            values.reshape(half_rows, items, V_DIM),
            ropes,
        )
    ]
    borders = jnp.sum((segments == 0).astype(jnp.int32), axis=1)
    mine = jnp.arange(stream_count, dtype=jnp.int32) == lax.axis_index(EXPERT) // HEADS
    bound = jnp.sum(jnp.where(mine, borders, 0)).reshape(1)
    own_weights = (expert_gate[0].T, expert_up[0].T, expert_down[0])
    table = column_table(
        by_stream(routes[0, 0]), by_stream(route_weights[0, 0]), expert_count, lax.axis_size("z")
    )
    attn_rows, weight_table, other_weights, proj_all = attend_and_gather(
        packed, bound, table, out_proj, own_weights
    )
    projected = jnp.dot(
        attn_rows, proj_all.reshape(model_width, model_width), preferred_element_type=jnp.float32
    )
    hidden = by_stream(residual).astype(jnp.float32) + projected
    mean_square = jnp.mean(hidden * hidden, axis=1, keepdims=True)
    normed = (hidden * lax.rsqrt(mean_square + EPSILON) * norm_gain.astype(jnp.float32)).astype(
        jnp.bfloat16
    )
    layer_out = mix_experts(normed, hidden, weight_table, own_weights, other_weights)
    return jnp.swapaxes(layer_out.reshape(stream_count, half_rows, model_width), 0, 1)


def solution(mesh):
    split = Mesh(mesh.devices.reshape(4, 2, 4, 8), DP + EXPERT)
    rows = P(EXPERT, DP, None)
    weights = P(EXPERT, None, None)
    pairs = P(DP, EXPERT, None, None)
    return jax.shard_map(
        body,
        mesh=split,
        in_specs=(
            rows,
            rows,
            rows,
            rows,
            rows,
            P(DP, None),
            P(DP + EXPERT, None),
            P(),
            weights,
            weights,
            weights,
            pairs,
            pairs,
        ),
        out_specs=rows,
        check_vma=False,
    )
```

```python
import functools

import jax
import jax.numpy as jnp
from jax import lax
from jax.experimental import pallas as pl
from jax.experimental.pallas import tpu as pltpu
from jax.sharding import Mesh, PartitionSpec as P

MESH = pl.DeviceIdType.MESH
DP = ("x", "core")
EXPERT = ("y", "z")

HEADS = 16
NOPE = 128
ROPE = 64
V_DIM = 128
TOP = 6


EPSILON = 1e-06
QUERY_BLOCK = 512


def front_kernel(queries, keys, values, ropes, bound, table, proj, own_g, own_u, own_d,
                 attn_ref, tab_ref, others, proj_all,
                 rows_buf, qbuf, kbuf, att, local_sem, a2a_sem, att_sem, tab_sem,
                 ysend, yrecv, xsend, xrecv, csend, crecv, psend, precv):
    size_x, size_y, size_z = lax.axis_size("x"), lax.axis_size("y"), lax.axis_size("z")
    peers = size_y * size_z
    x, core = lax.axis_index("x"), lax.axis_index("core")
    y, z = lax.axis_index("y"), lax.axis_index("z")
    me = y * size_z + z
    up_y, down_y = {"y": lax.rem(y + 1, size_y)}, {"y": lax.rem(y + size_y - 1, size_y)}
    up_x, down_x = {"x": lax.rem(x + 1, size_x)}, {"x": lax.rem(x + size_x - 1, size_x)}
    other_core = {"core": 1 - core}
    packed = (queries, keys, values, ropes)
    block = queries.shape[1]
    heads = attn_ref.shape[1] // V_DIM
    ff, width = own_d.shape
    high, wide = ff // size_x, width // 4

    def peer(e):
        return {"y": lax.div(e, size_z), "z": lax.rem(e, size_z)}

    def remote(src, dst, send, recv, device):
        return pltpu.make_async_remote_copy(
            src_ref=src, dst_ref=dst, send_sem=send, recv_sem=recv, device_id=device, device_id_type=MESH
        )

    barrier = pltpu.get_barrier_semaphore()

    def greet(d, carry):
        pl.semaphore_signal(barrier, inc=1, device_id=peer(lax.rem(me + d, peers)), device_id_type=MESH)
        return carry

    lax.fori_loop(1, peers, greet, 0)
    for device in (up_x, down_x, other_core):
        pl.semaphore_signal(barrier, inc=1, device_id=device, device_id_type=MESH)
    pl.semaphore_wait(barrier, peers + 2)

    def blocks(first, amount):
        return proj_all.at[pl.ds(first, amount)]

    own_block = ((x * 2 + core) * size_y + y) * size_z + z
    group = peers

    def group_of(gx, gcore):
        return (lax.rem(gx + size_x, size_x) * 2 + gcore) * group

    def proj_copy(n, first, amount, device):
        return remote(blocks(first, amount), blocks(first, amount), psend.at[n], precv.at[n], device)

    for d in range(1, size_z):
        remote(proj, proj_all.at[own_block], psend.at[0], precv.at[0], {"z": lax.rem(z + d, size_z)}).start()
    own_proj = pltpu.make_async_copy(proj, proj_all.at[own_block], local_sem.at[3])
    own_proj.start()

    def rows_of(e):
        return pl.ds(pl.multiple_of(e * block, block), block)

    def send_rows(d, carry):
        e = lax.rem(me + d, peers)
        for i, part in enumerate(packed):
            place = rows_buf.at[rows_of(me), pl.ds(i * 128, 128)]
            remote(part.at[e], place, a2a_sem.at[0], a2a_sem.at[1], peer(e)).start()
        return carry

    lax.fori_loop(1, peers, send_rows, 0)
    for i, part in enumerate(packed):
        place = rows_buf.at[rows_of(me), pl.ds(i * 128, 128)]
        pltpu.make_async_copy(part.at[me], place, local_sem.at[0]).start()

    own_proj.wait()
    proj_copy(0, 0, size_z - 1, up_y).wait_recv()
    for d in range(1, size_y):
        proj_copy(1, own_block - z, size_z, {"y": lax.rem(y + d, size_y)}).start()

    def columns(u):
        return pl.ds(pl.multiple_of((core * 2 + u) * wide, wide), wide)

    def region(s, q, u):
        return others.at[s, :, pl.ds(q * high, high), columns(u)]

    def y_index(s, q, u):
        return (s * 2 + q) * 2 + u

    def y_start(s, q, u):
        n = y_index(s, q, u)
        quarter = pl.ds(pl.multiple_of(lax.rem(x + q, size_x) * high, high), high)
        for m, own in enumerate((own_g, own_u, own_d)):
            remote(
                own.at[quarter, columns(u)],
                others.at[s, m, pl.ds(q * high, high), columns(u)],
                ysend.at[n],
                yrecv.at[n],
                up_y if s == 0 else down_y,
            ).start()

    def y_copy(s, q, u):
        n = y_index(s, q, u)
        return remote(region(s, q, u), region(s, q, u), ysend.at[n], yrecv.at[n], up_y)

    def x_copy(s, q, u):
        device, slot = (up_x, 3) if q == 0 else (down_x, 2)
        n = (s * 2 + q) * 2 + u
        return remote(region(s, q, u), region(s, slot, u), xsend.at[n], xrecv.at[n], device)

    def c_copy(s, q, u):
        n = (s * 4 + q) * 2 + u
        return remote(region(s, q, u), region(s, q, u), csend.at[n], crecv.at[n], other_core)

    for first in (True, False):
        for u in range(2):
            for s in range(2):
                y_start(s, s if first else 1 - s, u)

    def tab_copy(d):
        to = lax.rem(z + d, size_z)
        return remote(table.at[to], tab_ref.at[z], tab_sem.at[0], tab_sem.at[1], {"z": to})

    for d in range(1, size_z):
        tab_copy(d).start()
    own_table = pltpu.make_async_copy(table.at[z], tab_ref.at[z], local_sem.at[1])
    own_table.start()

    proj_copy(1, 0, (size_y - 1) * size_z, up_y).wait_recv()
    for n, device in ((2, up_x), (3, down_x), (4, other_core)):
        proj_copy(n, group_of(x, core), group, device).start()

    def arrived(s, q, u):
        if s == 0:
            x_copy(s, q, u).start()
            c_copy(s, q, u).start()

    for s in range(2):
        y_copy(s, s, 0).wait_recv()
        arrived(s, s, 0)

    own_place = rows_buf.at[rows_of(me)]
    pltpu.make_async_copy(own_place, own_place, local_sem.at[0]).wait()
    most = rows_buf.at[pl.ds(0, (peers - 1) * block)]
    remote(most, most, a2a_sem.at[0], a2a_sem.at[1], up_y).wait_recv()

    length = rows_buf.shape[0]
    lane = lax.broadcasted_iota(jnp.int32, (1, 128), 1)
    swap = (
        lax.broadcasted_iota(jnp.int32, (128, 128), 0) == lax.broadcasted_iota(jnp.int32, (128, 128), 1) + ROPE
    ).astype(jnp.bfloat16)

    step = min(512, length)
    strip = min(256, step)

    def arrange(i, carry):
        span = pl.ds(pl.multiple_of(i * step, step), step)
        rope = rows_buf[span, 384:512]
        qbuf[span, 0:128] = rows_buf[span, 0:128]
        qbuf[span, 128:256] = jnp.where(lane < ROPE, rope, jnp.zeros_like(rope))
        kbuf[span, 0:128] = rows_buf[span, 128:256]
        kbuf[span, 128:256] = jnp.dot(rope, swap, preferred_element_type=jnp.float32).astype(jnp.bfloat16)
        return carry

    lax.fori_loop(0, length // step, arrange, 0)
    border = bound[0]
    scale = (NOPE + ROPE) ** (-0.5)
    stream, head = lax.div(me, heads), lax.rem(me, heads)
    target = (
        pl.ds(pl.multiple_of(stream * block, block), block),
        pl.ds(pl.multiple_of(head * V_DIM, V_DIM), V_DIM),
    )

    def back_copy(e):
        return remote(att.at[rows_of(e)], attn_ref.at[target[0], target[1]], att_sem.at[0], att_sem.at[1], peer(e))

    def local_back():
        return pltpu.make_async_copy(att.at[rows_of(me)], attn_ref.at[target[0], target[1]], local_sem.at[2])

    def attend(i):
        limit = (i + 1) * step

        def one(j, carry):
            first = i * step + j * strip
            span = pl.ds(pl.multiple_of(first, strip), strip)
            scores = lax.dot_general(
                qbuf[span, :], kbuf[0:limit, :], (((1,), (1,)), ((), ())), preferred_element_type=jnp.float32
            ) * scale
            row = first + lax.broadcasted_iota(jnp.int32, (strip, 1), 0)
            column = lax.broadcasted_iota(jnp.int32, (1, limit), 1)
            lowest = jnp.where(row >= border, border, 0)
            scores = jnp.where((column <= row) & (column >= lowest), scores, -jnp.inf)
            raised = jnp.exp(scores - jnp.max(scores, axis=1, keepdims=True))
            total = jnp.sum(raised, axis=1, keepdims=True)
            mixed = jnp.dot(
                raised.astype(jnp.bfloat16), rows_buf[0:limit, 256:384], preferred_element_type=jnp.float32
            )
            att[span, :] = (mixed / total).astype(jnp.bfloat16)
            for t in range(strip // block):
                e = lax.div(first, block) + t

                @pl.when(e != me)
                def _():
                    back_copy(e).start()

                @pl.when(e == me)
                def _():
                    local_back().start()

            return carry

        lax.fori_loop(0, step // strip, one, 0)

    count = length // step
    for i in range(count):
        attend(i)
        if i + 1 != (count + 1) // 2:
            continue
        half_group = group // 2
        proj_copy(2, group_of(x - 1, core), group, up_x).wait_recv()
        proj_copy(5, group_of(x - 1, core), half_group, up_x).start()
        proj_copy(7, group_of(x - 1, core), group, other_core).start()
        proj_copy(3, group_of(x + 1, core), group, up_x).wait_recv()
        proj_copy(6, group_of(x + 1, core) + half_group, half_group, down_x).start()
        proj_copy(8, group_of(x + 1, core), group, other_core).start()

    def crossed(s, q, u):
        x_copy(s, q, u).wait_recv()
        c_copy(s, 3 if q == 0 else 2, u).start()

    for s in range(2):
        y_copy(s, s, 1).wait_recv()
        arrived(s, s, 1)
    proj_copy(5, 0, half_group, up_x).wait_recv()
    proj_copy(9, group_of(x + 2, core), half_group, other_core).start()
    proj_copy(6, 0, half_group, up_x).wait_recv()
    proj_copy(10, group_of(x + 2, core) + half_group, half_group, other_core).start()
    for u in range(2):
        for s in range(2):
            y_copy(s, 1 - s, u).wait_recv()
            arrived(s, 1 - s, u)
    for u in range(2):
        crossed(0, 0, u)
    for u in range(2):
        crossed(0, 1, u)

    for q in range(4):
        for u in range(2):
            c_copy(0, q, u).wait()
    for u in range(2):
        for q in range(2):
            for s in range(2):
                y_copy(s, q, u).wait_send()
            x_copy(0, q, u).wait_send()
    proj_copy(0, 0, size_z - 1, up_y).wait_send()
    proj_copy(1, 0, (size_y - 1) * size_z, up_y).wait_send()
    for n, amount in ((2, group), (3, group), (5, half_group), (6, half_group)):
        proj_copy(n, 0, amount, up_x).wait_send()
    for n, amount in ((4, group), (7, group), (8, group), (9, half_group), (10, half_group)):
        proj_copy(n, 0, amount, other_core).wait()
    remote(most, most, a2a_sem.at[0], a2a_sem.at[1], up_y).wait_send()
    local_back().wait()
    back = att.at[pl.ds(0, (peers - 1) * block)]
    remote(back, back, att_sem.at[0], att_sem.at[1], up_y).wait()
    own_table.wait()
    tables = tab_ref.at[pl.ds(0, size_z - 1)]
    remote(tables, tables, tab_sem.at[0], tab_sem.at[1], up_y).wait()


def attend_and_gather(packed, bound, table, proj, own_weights):
    peers, block, _ = packed[0].shape
    ff, width = own_weights[2].shape
    heads = width // V_DIM
    length = peers * block
    vmem = pl.BlockSpec(memory_space=pltpu.VMEM)
    anywhere = pl.BlockSpec(memory_space=pl.ANY)
    dma = pltpu.SemaphoreType.DMA
    return pl.pallas_call(
        front_kernel,
        out_shape=(
            jax.ShapeDtypeStruct((peers // heads * block, width), jnp.bfloat16),
            jax.ShapeDtypeStruct(table.shape, jnp.float32),
            jax.ShapeDtypeStruct((2, 3, ff, width), jnp.bfloat16),
            jax.ShapeDtypeStruct((width // proj.shape[0],) + proj.shape, jnp.bfloat16),
        ),
        in_specs=[anywhere] * 4 + [pl.BlockSpec(memory_space=pltpu.SMEM), vmem] + [anywhere] * 4,
        out_specs=(vmem, vmem, anywhere, anywhere),
        scratch_shapes=[
            pltpu.VMEM((length, 512), jnp.bfloat16),
            pltpu.VMEM((length, 256), jnp.bfloat16),
            pltpu.VMEM((length, 256), jnp.bfloat16),
            pltpu.VMEM((length, V_DIM), jnp.bfloat16),
            dma((4,)),
            dma((2,)),
            dma((2,)),
            dma((2,)),
            dma((8,)),
            dma((8,)),
            dma((4,)),
            dma((4,)),
            dma((8,)),
            dma((8,)),
            dma((11,)),
            dma((11,)),
        ],
        compiler_params=pltpu.CompilerParams(
            collective_id=1, has_side_effects=True, vmem_limit_bytes=50000000
        ),
        cost_estimate=pl.CostEstimate(flops=100000000000, bytes_accessed=40000000, transcendentals=0),
    )(*packed, bound, table, proj, *own_weights)


def moe_kernel(axis_size, x_ref, hid_ref, wt_ref, own_g, own_u, own_d, others,
               out_ref, xbuf, acc, act, weights, rbuf, lbuf, start_sem, send_sem, recv_sem, wsem,
               fsend, frecv, xsend, xrecv, csend, crecv, lsem):
    n = axis_size
    half_n = n // 2
    y, z = lax.axis_index("y"), lax.axis_index("z")
    right = {"z": lax.rem(z + 1, n)}
    left = {"z": lax.rem(z + n - 1, n)}
    rows = x_ref.shape[0]
    half = rows // 2
    count, _, ff, width = weights.shape
    sent = 2 * half_n - 1

    def slot(d):
        return lax.rem(z + 2 * n - d, n)

    def part(c):
        return pl.ds(pl.multiple_of(c * half, half), half)

    for i, own in enumerate((own_g, own_u, own_d)):
        pltpu.make_async_copy(own, weights.at[0, i], wsem.at[0]).start()
    first_late = count - 2
    for k in range(1, first_late):
        pltpu.make_async_copy(others.at[k - 1], weights.at[k], wsem.at[k]).start()

    size_x, size_y = lax.axis_size("x"), lax.axis_size("y")
    x, core = lax.axis_index("x"), lax.axis_index("core")
    up_y, down_y = {"y": lax.rem(y + 1, size_y)}, {"y": lax.rem(y + size_y - 1, size_y)}
    up_x, down_x = {"x": lax.rem(x + 1, size_x)}, {"x": lax.rem(x + size_x - 1, size_x)}
    other_core = {"core": 1 - core}
    barrier = pltpu.get_barrier_semaphore()
    for neighbour in (left, right, up_y, down_y, up_x, down_x, other_core):
        pl.semaphore_signal(barrier, inc=1, device_id=neighbour, device_id_type=MESH)
    pl.semaphore_wait(barrier, 7)

    def gather_copy(j, way):
        d = j // 2
        c = lax.rem(j + way, 2)
        source = slot(d) if way == 0 else slot(n - d)
        return pltpu.make_async_remote_copy(
            src_ref=xbuf.at[source, part(c)],
            dst_ref=xbuf.at[source, part(c)],
            send_sem=send_sem.at[way, j],
            recv_sem=recv_sem.at[way, j],
            device_id=right if way == 0 else left,
            device_id_type=MESH,
        )

    def gather_arrival(j, way):
        d = j // 2 + 1
        c = lax.rem(j + way, 2)
        source = slot(d) if way == 0 else slot(n - d)
        return pltpu.make_async_remote_copy(
            src_ref=xbuf.at[source, part(c)],
            dst_ref=xbuf.at[source, part(c)],
            send_sem=send_sem.at[way, j],
            recv_sem=recv_sem.at[way, j],
            device_id=right if way == 0 else left,
            device_id_type=MESH,
        )

    own_copy = pltpu.make_async_copy(x_ref, xbuf.at[z], start_sem)
    own_copy.start()
    own_copy.wait()
    for j in range(2):
        for way in range(2):
            gather_copy(j, way).start()

    high, wide = ff // size_x, width // 4
    near, far_k = count - 2, count - 1

    def section(ref, k, q, u):
        columns = pl.ds(pl.multiple_of((core * 2 + u) * wide, wide), wide)
        return ref.at[k, :, pl.ds(q * high, high), columns]

    def remote(src, dst, send, recv, device):
        return pltpu.make_async_remote_copy(
            src_ref=src, dst_ref=dst, send_sem=send, recv_sem=recv, device_id=device, device_id_type=MESH
        )

    def origin(k, q, u):
        return section(others, 1, q, u) if k == near and q < 2 else section(weights, k, q, u)

    def f_copy(q, u):
        n = q * 2 + u
        return remote(
            section(others, q, q, u), section(weights, far_k, q, u), fsend.at[n], frecv.at[n],
            up_y if q == 0 else down_y,
        )

    def x_copy(k, q, u):
        n = ((k - near) * 2 + q) * 2 + u
        device, slot = (up_x, 3) if q == 0 else (down_x, 2)
        return remote(origin(k, q, u), section(weights, k, slot, u), xsend.at[n], xrecv.at[n], device)

    def c_copy(k, q, u):
        n = ((k - near) * 4 + q) * 2 + u
        return remote(origin(k, q, u), section(weights, k, q, u), csend.at[n], crecv.at[n], other_core)

    def local_copy(q, u):
        return pltpu.make_async_copy(section(others, 1, q, u), section(weights, near, q, u), lsem.at[q * 2 + u])

    def arrived(u):
        for q in range(2):
            f_copy(q, u).wait_recv()
            x_copy(far_k, q, u).start()
            c_copy(far_k, q, u).start()

    def crossed(k, u):
        for q in range(2):
            x_copy(k, q, u).wait_recv()
            c_copy(k, 3 if q == 0 else 2, u).start()

    for u in range(2):
        for q in range(2):
            f_copy(q, u).start()
            x_copy(near, q, u).start()
            c_copy(near, q, u).start()
            local_copy(q, u).start()

    def pass_on(j):
        for way in range(2):
            gather_arrival(j, way).wait_recv()

        @pl.when(j + 2 < sent)
        def _():
            for way in range(2):
                gather_copy(j + 2, way).start()

    lanes = lax.broadcasted_iota(jnp.int32, (1, wt_ref.shape[2]), 1)
    cuts = [(a, min(a + 256, ff)) for a in range(0, ff, 256)]

    def gate_up(slots, k):
        x = jnp.concatenate([xbuf[s] for s in slots], axis=0) if len(slots) > 1 else xbuf[slots[0]]
        wrow = jnp.concatenate([wt_ref[s] for s in slots], axis=0) if len(slots) > 1 else wt_ref[slots[0]]
        offset = jnp.where(k == 0, 0, jnp.where(k == 1, count - 1, k - 1))
        scale = jnp.sum(jnp.where(lanes == lax.rem(y + offset, count), wrow, 0.0), axis=1, keepdims=True)
        m = x.shape[0]

        def product(which, lo, hi):
            return lax.dot_general(
                x, weights[k, which, lo:hi], (((1,), (1,)), ((), ())), preferred_element_type=jnp.float32
            )

        for lo, hi in cuts:
            g, u = product(0, lo, hi), product(1, lo, hi)
            a = g / (1.0 + jnp.exp(-g)) * u * scale
            act[k, 0:m, lo:hi] = a.astype(jnp.bfloat16)

    def down(slots, experts, more):
        m = rows * len(slots)

        def columns(q, carry):
            span = pl.ds(pl.multiple_of(q * 512, min(512, width)), min(512, width))
            y = jnp.dot(act[experts[0], 0:m, :], weights[experts[0], 2, :, span], preferred_element_type=jnp.float32)
            for k in experts[1:]:
                y += jnp.dot(act[k, 0:m, :], weights[k, 2, :, span], preferred_element_type=jnp.float32)
            for i, s in enumerate(slots):
                part_y = y[i * rows:(i + 1) * rows]
                if more:
                    part_y += acc[s, :, span].astype(jnp.float32)
                acc[s, :, span] = part_y.astype(jnp.bfloat16)
            return carry

        lax.fori_loop(0, max(1, width // 512), columns, 0)

    def fetched(k):
        whole = weights.at[k]
        pltpu.make_async_copy(whole, whole, wsem.at[k]).wait()

    def own_step(k, carry):
        fetched(k)
        gate_up([z], k)

        @pl.when(k == 1)
        def _():
            pass_on(0)

        return carry

    early, late = tuple(range(near)), (near, far_k)
    lax.fori_loop(0, near, own_step, 0)
    down([z], early, False)
    crossed(near, 0)
    arrived(0)

    def pair_step(p, carry):
        pass_on(2 * p - 1)
        slots = [slot(p), slot(n - p)]

        def one(k, inner):
            gate_up(slots, k)

            @pl.when(k == 1)
            def _():
                pass_on(2 * p)

            return inner

        lax.fori_loop(0, near, one, 0)
        down(slots, early, False)

        @pl.when(p == 1)
        def _():
            crossed(near, 1)
            arrived(1)

        @pl.when(p == 2)
        def _():
            crossed(far_k, 0)

        @pl.when(p == 3)
        def _():
            crossed(far_k, 1)

        return carry

    lax.fori_loop(1, half_n, pair_step, 0)
    far = [slot(half_n)]

    def far_step(k, carry):
        gate_up(far, k)
        return carry

    lax.fori_loop(0, near, far_step, 0)
    down(far, early, False)
    for q in range(4):
        for u in range(2):
            c_copy(near, q, u).wait_recv()
            if q < 2:
                local_copy(q, u).wait()

    def finish(slots, ready=True):
        gate_up(slots, near)
        if not ready:
            for q in range(4):
                for u in range(2):
                    c_copy(far_k, q, u).wait_recv()
        gate_up(slots, far_k)
        down(slots, late, True)

    finish(far, False)
    bufs = (rbuf, lbuf)

    def sum_copy(j, way):
        return pltpu.make_async_remote_copy(
            src_ref=bufs[way].at[sent + j if j < 2 else j - 2],
            dst_ref=bufs[way].at[j],
            send_sem=send_sem.at[way, sent + j],
            recv_sem=recv_sem.at[way, sent + j],
            device_id=right if way == 0 else left,
            device_id_type=MESH,
        )

    def send_sums(j):
        for way in range(2):
            off = half_n - (j + 1) // 2
            owner = slot(n - off) if way == 0 else slot(off)
            c = (j + way) % 2
            own_part = acc[owner, part(c)]
            if j < 2:
                bufs[way][sent + j] = own_part
            else:
                sum_copy(j - 2, way).wait_recv()
                bufs[way][j - 2] = (bufs[way][j - 2].astype(jnp.float32) + own_part.astype(jnp.float32)).astype(jnp.bfloat16)
            sum_copy(j, way).start()

    send_sums(0)
    for p in range(half_n - 1, 0, -1):
        finish([slot(p), slot(n - p)])
        j = 2 * (half_n - p) - 1
        send_sums(j)
        send_sums(j + 1)
    finish([z])
    for way in range(2):
        for j in (sent - 2, sent - 1):
            sum_copy(j, way).wait_recv()
    for c in range(2):
        total = hid_ref[part(c)] + acc[z, part(c)].astype(jnp.float32)
        for way in range(2):
            j = sent - 1 if (sent - 1 + way) % 2 == c else sent - 2
            total += bufs[way][j].astype(jnp.float32)
        out_ref[part(c)] = total.astype(jnp.bfloat16)
    for j in range(sent):
        for way in range(2):
            gather_copy(j, way).wait_send()
            sum_copy(j, way).wait_send()
    for u in range(2):
        for k in late:
            for q in range(4):
                c_copy(k, q, u).wait_send()
            for q in range(2):
                x_copy(k, q, u).wait_send()
        for q in range(2):
            f_copy(q, u).wait_send()


def mix_experts(normed, hidden, weight_table, own_weights, other_weights):
    rows, width = normed.shape
    n = lax.axis_size("z")
    ff = own_weights[2].shape[0]
    count = 2 + other_weights.shape[0]
    sent = n - 1
    vmem = pl.BlockSpec(memory_space=pltpu.VMEM)
    anywhere = pl.BlockSpec(memory_space=pl.ANY)
    return pl.pallas_call(
        functools.partial(moe_kernel, n),
        out_shape=jax.ShapeDtypeStruct((rows, width), jnp.bfloat16),
        in_specs=[vmem] * 3 + [anywhere] * 4,
        out_specs=vmem,
        scratch_shapes=[
            pltpu.VMEM((n, rows, width), jnp.bfloat16),
            pltpu.VMEM((n, rows, width), jnp.bfloat16),
            pltpu.VMEM((count, 2 * rows, ff), jnp.bfloat16),
            pltpu.VMEM((count, 3, ff, width), jnp.bfloat16),
            pltpu.VMEM((sent + 2, rows // 2, width), jnp.bfloat16),
            pltpu.VMEM((sent + 2, rows // 2, width), jnp.bfloat16),
            pltpu.SemaphoreType.DMA,
            pltpu.SemaphoreType.DMA((2, 2 * sent)),
            pltpu.SemaphoreType.DMA((2, 2 * sent)),
            pltpu.SemaphoreType.DMA((count,)),
        ] + [pltpu.SemaphoreType.DMA((amount,)) for amount in (4, 4, 8, 8, 16, 16, 4)] + [
        ],
        compiler_params=pltpu.CompilerParams(
            collective_id=0, has_side_effects=True, vmem_limit_bytes=66000000
        ),
        cost_estimate=pl.CostEstimate(
            flops=6 * n * rows * width * ff * count, bytes_accessed=40000000, transcendentals=0
        ),
    )(normed, hidden, weight_table, *own_weights, other_weights)


def column_table(routes, route_weights, expert_count, n):
    experts = jnp.arange(expert_count, dtype=jnp.int32)
    chosen = routes[:, :, None] == experts[None, None, :]
    table = jnp.sum(jnp.where(chosen, route_weights[:, :, None], 0.0), axis=1)
    return jnp.transpose(table.reshape(table.shape[0], expert_count // n, n), (2, 0, 1))


def body(
    queries,
    key_nope,
    key_rope,
    values,
    residual,
    segments,
    out_proj,
    norm_gain,
    expert_gate,
    expert_up,
    expert_down,
    routes,
    route_weights,
):
    half_rows, stream_count, _ = queries.shape
    model_width = residual.shape[2]
    token_rows = half_rows * stream_count
    expert_count = lax.axis_size(EXPERT)
    items = stream_count * HEADS

    def by_stream(array):
        array = array.reshape(half_rows, stream_count, array.shape[-1])
        return jnp.swapaxes(array, 0, 1).reshape(token_rows, array.shape[-1])

    query_items = queries.reshape(half_rows, items, NOPE + ROPE)
    rope_items = jnp.broadcast_to(key_rope[:, :, None, :], (half_rows, stream_count, HEADS, ROPE))
    ropes = jnp.concatenate(
        [query_items[:, :, NOPE:], rope_items.reshape(half_rows, items, ROPE)], axis=2
    )
    packed = [
        jnp.swapaxes(part, 0, 1)
        for part in (
            query_items[:, :, :NOPE],
            key_nope.reshape(half_rows, items, NOPE),
            values.reshape(half_rows, items, V_DIM),
            ropes,
        )
    ]
    borders = jnp.sum((segments == 0).astype(jnp.int32), axis=1)
    mine = jnp.arange(stream_count, dtype=jnp.int32) == lax.axis_index(EXPERT) // HEADS
    bound = jnp.sum(jnp.where(mine, borders, 0)).reshape(1)
    own_weights = (expert_gate[0].T, expert_up[0].T, expert_down[0])
    table = column_table(
        by_stream(routes[0, 0]), by_stream(route_weights[0, 0]), expert_count, lax.axis_size("z")
    )
    attn_rows, weight_table, other_weights, proj_all = attend_and_gather(
        packed, bound, table, out_proj, own_weights
    )
    projected = jnp.dot(
        attn_rows, proj_all.reshape(model_width, model_width), preferred_element_type=jnp.float32
    )
    hidden = by_stream(residual).astype(jnp.float32) + projected
    mean_square = jnp.mean(hidden * hidden, axis=1, keepdims=True)
    normed = (hidden * lax.rsqrt(mean_square + EPSILON) * norm_gain.astype(jnp.float32)).astype(
        jnp.bfloat16
    )
    layer_out = mix_experts(normed, hidden, weight_table, own_weights, other_weights)
    return jnp.swapaxes(layer_out.reshape(stream_count, half_rows, model_width), 0, 1)


def solution(mesh):
    split = Mesh(mesh.devices.reshape(4, 2, 4, 8), DP + EXPERT)
    rows = P(EXPERT, DP, None)
    weights = P(EXPERT, None, None)
    pairs = P(DP, EXPERT, None, None)
    return jax.shard_map(
        body,
        mesh=split,
        in_specs=(
            rows,
            rows,
            rows,
            rows,
            rows,
            P(DP, None),
            P(DP + EXPERT, None),
            P(),
            weights,
            weights,
            weights,
            pairs,
            pairs,
        ),
        out_specs=rows,
        check_vma=False,
    )
```
